128 devices in a mesh: section: 2 (over y_lo), row: 4 (over y_hi, core), col: 16 (over x, z).
Axes of the slice: x: 4, y: 4 (y_hi: 2, y_lo: 2; y = y_hi * 2 + y_lo), z: 4, core: 2. Of those that a mesh axis runs over, the one named last changes fastest.
Arguments:
- stash_inputs: bfloat16 [2, 4, 512, 12288], P('section', None, 'row', 'col'), may hold values from -16 to 16
- stash_hidden: bfloat16 [2, 4, 512, 24576], P('section', None, 'col', 'row'), may hold values from -6 to 6
- grad_in: bfloat16 [2, 512, 12288], P('section', 'row', 'col'), may hold values from -6 to 6
- w_in: bfloat16 [2, 12288, 24576], P('section', 'col', 'row'), may hold values from -0.0546875 to 0.0546875
- b_in: float32 [2, 24576], P('section', 'row'), may hold values from -3 to 3
- w_out: bfloat16 [2, 24576, 12288], P('section', 'row', 'col'), may hold values from -0.0390625 to 0.0390625
- b_out: float32 [2, 12288], P('section', 'col'), may hold values from -3 to 3
- ln_gain: float32 [2, 12288], P('section', 'col'), may hold values from 0.4 to 1.6
- plan: int32 [2, 2], P('section'), may hold values from 0 to 3, as said below
Outputs:
- act_recv: bfloat16 [2, 512, 12288], P('section', 'row', 'col')
- grad_recv: bfloat16 [2, 512, 12288], P('section', 'row', 'col')
- saved_hidden: bfloat16 [2, 512, 24576], P('section', 'col', 'row')
The draws below stay inside these ranges and needn't reach their ends.
Inputs may be any that keep to these rules, and one draw needn't show every extreme that they name: plan[s, 0] is the stash slot of the micro-batch that section s takes backward, plan[s, 1] that of the one it takes forward; the two differ.
All inputs are finite; a program needn't handle non-finite values.
Results may differ from the reference program's by a relative error of at most 0.015.
Values may be sent and summed in bfloat16 or wider, within the bound.
A program may use at most 128 MiB of HBM per device.

```python
import jax
import jax.numpy as jnp
from jax import lax

D = 12288
FF = 24576
TOK = 512
STASH = 4
N_SECTION = 2


def draw_stash_inputs(key, part):
    key_noise = jax.random.fold_in(key, 11)
    key_cols = jax.random.fold_in(key, 12)
    ramp = jnp.arange(D, dtype=jnp.float32) / D
    col_scale = jnp.exp(ramp * jnp.log(3.0) + jax.random.uniform(key_cols, (D,), jnp.float32, 0.0, jnp.log(4.0))) / 6.0
    noise = jnp.clip(jax.random.normal(key_noise, (N_SECTION, STASH, TOK, D), jnp.float32), -6.0, 6.0)
    values = noise * col_scale
    return values.astype(jnp.bfloat16)


def draw_plan(key, part):
    key_back = jax.random.fold_in(key, 21)
    key_step = jax.random.fold_in(key, 22)
    back_slot = jax.random.randint(key_back, (N_SECTION,), 0, STASH)
    step_size = jax.random.randint(key_step, (N_SECTION,), 1, STASH)
    fwd_slot = (back_slot + step_size) % STASH
    return jnp.stack([back_slot, fwd_slot], axis=1).astype(jnp.int32)


def levels(own_key, dims, pieces, smallest, largest):
    level = 1.0
    for dim, shards_of in pieces:
        steps = jax.random.uniform(jax.random.fold_in(jax.random.fold_in(own_key, 6), dim), (shards_of,), jnp.float32, smallest / len(pieces), largest / len(pieces))
        level = level * jnp.repeat(jnp.exp(steps), dims[dim] // shards_of).reshape((-1,) + (1,) * (len(dims) - 1 - dim))
    return level


def scatter_about(rng, shape, width, limit, pieces=(), held_as=jnp.bfloat16):
    drawn = jax.random.normal(rng, shape, jnp.float32) * width
    if len(pieces) > 0:
        drawn = levels(rng, shape, pieces, -0.22, 0.18) * drawn
    return jnp.clip(drawn, min=-limit, max=limit).astype(held_as)


def setup_inputs(seed: int = 0) -> dict:
    arg_keys = jax.random.split(jax.random.key(seed), 10)
    return {
        "stash_inputs": draw_stash_inputs(jax.random.fold_in(arg_keys[9], 71), 0),
        "stash_hidden": scatter_about(arg_keys[1], (N_SECTION, STASH, TOK, FF), 1.5, 6.0, ((0, 2), (2, 16), (3, 4))),
        "grad_in": scatter_about(arg_keys[2], (N_SECTION, TOK, D), 1.0, 6.0, ((0, 2), (1, 4), (2, 16))),
        "w_in": scatter_about(arg_keys[3], (N_SECTION, D, FF), D ** -0.5, 0.0546875, ((0, 2), (1, 16), (2, 4))),
        "b_in": scatter_about(arg_keys[4], (N_SECTION, FF), 0.5, 3.0, ((0, 2), (1, 4)), jnp.float32),
        "w_out": scatter_about(arg_keys[5], (N_SECTION, FF, D), FF ** -0.5, 0.0390625, ((0, 2), (1, 4), (2, 16))),
        "b_out": scatter_about(arg_keys[6], (N_SECTION, D), 0.5, 3.0, ((0, 2), (1, 16)), jnp.float32),
        "ln_gain": jnp.clip(1.0 + 0.12 * jax.random.normal(arg_keys[7], (N_SECTION, D), jnp.float32), 0.4, 1.6),
        "plan": draw_plan(jax.random.fold_in(arg_keys[9], 71), 0),
    }


epsilon = 1e-05
root_coef = 0.7978845608028654
cubic_coef = 0.044715

def gelu_value(values):
    inner = root_coef * (values + cubic_coef * values * values * values)
    return 0.5 * values * (1.0 + jnp.tanh(inner))

def gelu_slope(values):
    inner = root_coef * (values + cubic_coef * values * values * values)
    tangent = jnp.tanh(inner)
    return 0.5 * (1.0 + tangent) + 0.5 * values * (1.0 - tangent * tangent) * root_coef * (1.0 + 3.0 * cubic_coef * values * values)

def finish_norm(values, total, squares):
    mean_val = total / D
    sq_mean = squares / D
    inv_std = lax.rsqrt(sq_mean - mean_val * mean_val + epsilon)
    return ((values - mean_val[:, None]) * inv_std[:, None], inv_std)

def transposed(left, right):
    return lax.dot_general(left, right, (((1,), (1,)), ((), ())), preferred_element_type=jnp.float32)

def section_step(fwd_input, bwd_input, bwd_hidden, upstream, w_first, b_first, w_second, b_second, gain_part):
    fwd_hat, fwd_inv = finish_norm(fwd_input, lax.optimization_barrier(jnp.sum(fwd_input, axis=1)), lax.optimization_barrier(jnp.sum(fwd_input * fwd_input, axis=1)))
    bwd_hat, bwd_inv = finish_norm(bwd_input, lax.optimization_barrier(jnp.sum(bwd_input, axis=1)), lax.optimization_barrier(jnp.sum(bwd_input * bwd_input, axis=1)))
    normed = (fwd_hat * gain_part).astype(jnp.bfloat16)
    hidden = jnp.dot(normed, w_first, preferred_element_type=jnp.float32) + b_first
    saved = hidden.astype(jnp.bfloat16)
    activated = gelu_value(hidden).astype(jnp.bfloat16)
    output = (jnp.dot(activated, w_second, preferred_element_type=jnp.float32) + b_second + fwd_input).astype(jnp.bfloat16)
    slopes = transposed(upstream, w_second)
    hid_grad = (slopes * gelu_slope(bwd_hidden)).astype(jnp.bfloat16)
    scaled = transposed(hid_grad, w_first) * gain_part
    first_mean = lax.optimization_barrier(jnp.sum(scaled, axis=1)) / D
    second_mean = lax.optimization_barrier(jnp.sum(scaled * bwd_hat, axis=1)) / D
    in_grad = upstream.astype(jnp.float32) + bwd_inv[:, None] * (scaled - first_mean[:, None] - bwd_hat * second_mean[:, None])
    return (output, in_grad.astype(jnp.bfloat16), saved)

def reference(stash_inputs, stash_hidden, grad_in, w_in, b_in, w_out, b_out, ln_gain, plan):
    outputs = []
    grads = []
    saves = []
    for section_id in range(N_SECTION):
        bwd_slot = plan[section_id, 0]
        fwd_slot = plan[section_id, 1]
        fwd_input = lax.dynamic_index_in_dim(stash_inputs[section_id], fwd_slot, 0, keepdims=False).astype(jnp.float32)
        bwd_input = lax.dynamic_index_in_dim(stash_inputs[section_id], bwd_slot, 0, keepdims=False).astype(jnp.float32)
        bwd_hidden = lax.dynamic_index_in_dim(stash_hidden[section_id], bwd_slot, 0, keepdims=False).astype(jnp.float32)
        output, in_grad, saved = section_step(fwd_input, bwd_input, bwd_hidden, grad_in[section_id], w_in[section_id], b_in[section_id], w_out[section_id], b_out[section_id], ln_gain[section_id])
        outputs.append(output)
        grads.append(in_grad)
        saves.append(saved)
    act_recv = jnp.stack([outputs[(section_id - 1) % N_SECTION] for section_id in range(N_SECTION)])
    grad_recv = jnp.stack([grads[(section_id + 1) % N_SECTION] for section_id in range(N_SECTION)])
    return (act_recv, grad_recv, jnp.stack(saves))
```

```python
import functools

import jax
import jax.numpy as jnp
from jax import lax
from jax.experimental import pallas as pl
from jax.experimental.pallas import tpu as pltpu
from jax.sharding import PartitionSpec as P

D = 12288
FT = 256
SIDE = 4
SLOTS = 8
SENDS = 4
BLK = 32

epsilon = 1e-05
root_coef = 0.7978845608028654
cubic_coef = 0.044715

RB1, D1, L1, RB2, D2, L2, A1, AR1, A2, AR2 = range(10)
KINDS = 10


def gelu_value(values):
    inner = root_coef * (values + cubic_coef * values * values * values)
    return 0.5 * values * (1.0 + jnp.tanh(inner))


def gelu_slope(values):
    inner = root_coef * (values + cubic_coef * values * values * values)
    tangent = jnp.tanh(inner)
    return 0.5 * (1.0 + tangent) + 0.5 * values * (1.0 - tangent * tangent) * root_coef * (
        1.0 + 3.0 * cubic_coef * values * values
    )


def dot_nn(a, b):
    return jnp.dot(a, b, preferred_element_type=jnp.float32)


def dot_nt(a, b):
    return lax.dot_general(a, b, (((1,), (1,)), ((), ())), preferred_element_type=jnp.float32)


def mid_kernel(
    lhs,
    stash,
    b_in,
    w_in,
    w_out,
    saved,
    out_fwd,
    out_bwd,
    win_s,
    wout_s,
    parts,
    rb1,
    lr1,
    quart,
    rb2,
    lr2,
    gath,
    acc,
    send_sem,
    recv_sem,
    win_sem,
    wout_sem,
):
    n_pair = win_s.shape[0] // 2
    ft = win_s.shape[2]
    units = 2 * n_pair
    f32, bf16 = jnp.float32, jnp.bfloat16
    col = lax.axis_index("col")
    pos = (col // SIDE, lax.rem(col, SIDE))

    def at_x(by):
        return {"col": lax.rem(pos[0] + by + SIDE, SIDE) * SIDE + pos[1]}

    def at_z(by):
        return {"col": pos[0] * SIDE + lax.rem(pos[1] + by + SIDE, SIDE)}

    hops = (at_x, at_z)

    def win_copy(t):
        return pltpu.make_async_copy(
            w_in.at[:, pl.ds(pl.multiple_of(t * ft, ft), ft)], win_s.at[t], win_sem.at[t]
        )

    def wout_copy(t):
        return pltpu.make_async_copy(
            w_out.at[pl.ds(pl.multiple_of(t * ft, ft), ft), :], wout_s.at[t], wout_sem.at[t]
        )

    @pl.loop(0, 2 * n_pair)
    def _(t):
        wout_copy(t).start()

    @pl.loop(0, 2 * n_pair)
    def _(t):
        win_copy(t).start()

    barrier = pltpu.get_barrier_semaphore()
    for hop in hops:
        for by in (1, -1):
            pl.semaphore_signal(
                barrier, inc=1, device_id=hop(by), device_id_type=pl.DeviceIdType.MESH
            )
    pl.semaphore_wait(barrier, 4)

    def ring(q, phase):
        axis = (q + phase) % 2
        return pos[axis], hops[axis]

    def wrap(v):
        return lax.rem(v + SIDE, SIDE)

    def copy(kind, q, u, d, src, dst, hop):
        return pltpu.make_async_remote_copy(
            src_ref=src,
            dst_ref=dst,
            send_sem=send_sem.at[kind, q, lax.rem(u, SENDS), d],
            recv_sem=recv_sem.at[kind, q, lax.rem(u, SLOTS), d],
            device_id=hop(1 if d == 0 else -1),
            device_id_type=pl.DeviceIdType.MESH,
        )

    def span(i, size, lo, n):
        return pl.ds(pl.multiple_of(i * size + lo, n), n)

    def scatter_copies(buf, back, side, size, kinds, me, hop, q, u):
        half = size // 2
        s = lax.rem(u, SLOTS)
        far, nxt, prv = wrap(me + 2), wrap(me + 1), wrap(me - 1)
        src = buf.at[q, s]
        relay = [
            copy(kinds[0], q, u, 0, src.at[span(far, size, 0, half)], back.at[q, s, 0], hop),
            copy(kinds[0], q, u, 1, src.at[span(far, size, half, half)], back.at[q, s, 1], hop),
        ]
        direct = [
            copy(kinds[1], q, u, 0, src.at[span(nxt, size, half, half)],
                 side.at[q, s, 0, pl.ds(half, half)], hop),
            copy(kinds[1], q, u, 1, src.at[span(prv, size, 0, half)],
                 side.at[q, s, 1, pl.ds(0, half)], hop),
        ]
        late = [
            copy(kinds[2], q, u, 0, src.at[span(nxt, size, 0, half)],
                 side.at[q, s, 0, pl.ds(0, half)], hop),
            copy(kinds[2], q, u, 1, src.at[span(prv, size, half, half)],
                 side.at[q, s, 1, pl.ds(half, half)], hop),
        ]
        return relay, direct, late

    def relay_step(buf, back, size, copies, me, q, u):
        relay, direct, late = copies
        half = size // 2
        s = lax.rem(u, SLOTS)
        for d, (chunk, lo) in enumerate(((wrap(me + 1), 0), (wrap(me - 1), half))):
            relay[d].wait_recv()
            rows = span(chunk, size, lo, half)
            buf[q, s, rows] = (
                buf[q, s, rows].astype(f32) + back[q, s, d].astype(f32)
            ).astype(bf16)
            late[d].start()
        for c in relay + direct:
            c.wait_send()

    big, small = SIDE * BLK, BLK

    def rs1(q, u):
        me, hop = ring(q, 0)
        return scatter_copies(parts, rb1, lr1, big, (RB1, D1, L1), me, hop, q, u)

    def rs2(q, u):
        me, hop = ring(q, 1)
        return scatter_copies(quart, rb2, lr2, small, (RB2, D2, L2), me, hop, q, u)

    def s0(u, q):
        s = lax.rem(u, SLOTS)

        @pl.when(u < n_pair)
        def _():
            t = 2 * u + q
            wout_copy(t).wait()
            parts[q, s] = dot_nt(lhs[0, q], wout_s[t]).astype(bf16)

        @pl.when(u >= n_pair)
        def _():
            t = 2 * (u - n_pair) + q
            parts[q, s] = dot_nn(lhs[1, q], win_s[t]).astype(bf16)

        relay, direct, _ = rs1(q, u)
        for c in relay + direct:
            c.start()

    def s1(u, q):
        me, _ = ring(q, 0)
        relay_step(parts, rb1, big, rs1(q, u), me, q, u)

    def s2(u, q):
        me, _ = ring(q, 0)
        s = lax.rem(u, SLOTS)
        _, direct, late = rs1(q, u)
        for c in direct + late:
            c.wait_recv()
        quart[q, s] = (
            parts[q, s, span(me, big, 0, big)].astype(f32)
            + lr1[q, s, 0].astype(f32)
            + lr1[q, s, 1].astype(f32)
        ).astype(bf16)
        relay, direct, _ = rs2(q, u)
        for c in relay + direct:
            c.start()
        for c in late:
            c.wait_send()

    def s3(u, q):
        me, _ = ring(q, 1)
        relay_step(quart, rb2, small, rs2(q, u), me, q, u)

    def gather1(q, u):
        me1, _ = ring(q, 0)
        me, hop = ring(q, 1)
        g = gath.at[q, lax.rem(u, SLOTS), me1]
        half = BLK // 2
        own = [copy(A1, q, u, d, g.at[me], g.at[me], hop) for d in (0, 1)]
        on = []
        for d, (b, lo) in enumerate(((wrap(me - 1), 0), (wrap(me + 1), half))):
            r = g.at[b, pl.ds(lo, half)]
            on.append(copy(AR1, q, u, d, r, r, hop))
        return own, on

    def gather2(q, u):
        me, hop = ring(q, 0)
        g = gath.at[q, lax.rem(u, SLOTS)]
        own = [copy(A2, q, u, d, g.at[me], g.at[me], hop) for d in (0, 1)]
        on = []
        for d, (b, lo) in enumerate(((wrap(me - 1), 0), (wrap(me + 1), SIDE // 2))):
            r = g.at[b, pl.ds(lo, SIDE // 2)]
            on.append(copy(AR2, q, u, d, r, r, hop))
        return own, on

    def s4(u, q):
        me1, _ = ring(q, 0)
        me2, _ = ring(q, 1)
        s = lax.rem(u, SLOTS)
        _, direct, late = rs2(q, u)
        for c in direct + late:
            c.wait_recv()
        h = (
            quart[q, s, span(me2, small, 0, small)].astype(f32)
            + lr2[q, s, 0].astype(f32)
            + lr2[q, s, 1].astype(f32)
        )

        @pl.when(u < n_pair)
        def _():
            t = 2 * u + q
            cols = pl.ds(pl.multiple_of(t * ft, ft), ft)
            slope = gelu_slope(stash[:, cols].astype(f32))
            gath[q, s, me1, me2] = (h * slope).astype(bf16)

        @pl.when(u >= n_pair)
        def _():
            t = 2 * (u - n_pair) + q
            cols = pl.ds(pl.multiple_of(t * ft, ft), ft)
            hidden = h + b_in[:, cols]
            saved[:, cols] = hidden.astype(bf16)
            gath[q, s, me1, me2] = gelu_value(hidden).astype(bf16)

        own, _ = gather1(q, u)
        for c in own:
            c.start()
        for c in late:
            c.wait_send()

    def pass_on(own, on):
        for d in (0, 1):
            own[d].wait_recv()
            on[d].start()
        for c in own:
            c.wait_send()

    def s5(u, q):
        pass_on(*gather1(q, u))

    def s6(u, q):
        _, on = gather1(q, u)
        for c in on:
            c.wait_recv()
        own, _ = gather2(q, u)
        for c in own:
            c.start()
        for c in on:
            c.wait_send()

    def s7(u, q):
        pass_on(*gather2(q, u))

    def s8(u, q):
        s = lax.rem(u, SLOTS)
        _, on = gather2(q, u)
        for c in on:
            c.wait_recv()
        for c in on:
            c.wait_send()
        rows = SIDE * SIDE * BLK
        piece = gath[q, s].reshape(rows, ft)

        def add(kind, first, value):
            @pl.when(first)
            def _():
                acc[kind, q] = value

            @pl.when(jnp.logical_not(first))
            def _():
                acc[kind, q] += value

        @pl.when(u < n_pair)
        def _():
            t = 2 * u + q
            win_copy(t).wait()
            add(0, u == 0, dot_nt(piece, win_s[t]))

        @pl.when(u >= n_pair)
        def _():
            t = 2 * (u - n_pair) + q
            add(1, u == n_pair, dot_nn(piece, wout_s[t]))

    stages = (s0, s1, s2, s3, s4, s5, s6, s7, s8)

    @pl.loop(0, units + len(stages) - 1)
    def _(step):
        for k, stage in enumerate(stages):
            u = step - k

            @pl.when(jnp.logical_and(u >= 0, u < units))
            def _():
                for q in (0, 1):
                    stage(u, q)

    @pl.loop(0, SIDE * SIDE)
    def _(b):
        x, z = b // SIDE, lax.rem(b, SIDE)
        rows = pl.ds(pl.multiple_of(b * BLK, BLK), BLK)
        swap = pl.ds(pl.multiple_of((z * SIDE + x) * BLK, BLK), BLK)
        out_bwd[rows] = (acc[0, 0, rows] + acc[0, 1, swap]).astype(out_bwd.dtype)
        out_fwd[rows] = (acc[1, 0, rows] + acc[1, 1, swap]).astype(out_fwd.dtype)


def mid(lhs, stash, b_in, w_in, w_out, ft=FT, out_dtype=jnp.bfloat16):
    feat, hid = w_in.shape
    tiles = hid // ft
    rows = SIDE * SIDE * BLK
    bf16 = jnp.bfloat16
    vmem, anyw = pl.BlockSpec(memory_space=pltpu.VMEM), pl.BlockSpec(memory_space=pl.ANY)
    flops = 8 * rows * feat * hid
    return pl.pallas_call(
        mid_kernel,
        out_shape=(
            jax.ShapeDtypeStruct((BLK, hid), bf16),
            jax.ShapeDtypeStruct((rows, feat), out_dtype),
            jax.ShapeDtypeStruct((rows, feat), out_dtype),
        ),
        in_specs=[vmem, vmem, vmem, anyw, anyw],
        out_specs=(vmem, vmem, vmem),
        scratch_shapes=[
            pltpu.VMEM((tiles, feat, ft), bf16),
            pltpu.VMEM((tiles, ft, feat), bf16),
            pltpu.VMEM((2, SLOTS, rows, ft), bf16),
            pltpu.VMEM((2, SLOTS, 2, 2 * BLK, ft), bf16),
            pltpu.VMEM((2, SLOTS, 2, 4 * BLK, ft), bf16),
            pltpu.VMEM((2, SLOTS, 4 * BLK, ft), bf16),
            pltpu.VMEM((2, SLOTS, 2, BLK // 2, ft), bf16),
            pltpu.VMEM((2, SLOTS, 2, BLK, ft), bf16),
            pltpu.VMEM((2, SLOTS, SIDE, SIDE, BLK, ft), bf16),
            pltpu.VMEM((2, 2, rows, feat), jnp.float32),
            pltpu.SemaphoreType.DMA((KINDS, 2, SENDS, 2)),
            pltpu.SemaphoreType.DMA((KINDS, 2, SLOTS, 2)),
            pltpu.SemaphoreType.DMA((tiles,)),
            pltpu.SemaphoreType.DMA((tiles,)),
        ],
        compiler_params=pltpu.CompilerParams(
            collective_id=0, has_side_effects=True, vmem_limit_bytes=67043328
        ),
        cost_estimate=pl.CostEstimate(
            flops=flops, bytes_accessed=4 * feat * hid, transcendentals=0
        ),
        name="mid",
    )(lhs, stash, b_in, w_in, w_out)


def copy_for_each(array, axis):
    copies = jnp.broadcast_to(array, (lax.axis_size(axis), *array.shape))
    return lax.all_to_all(copies, axis, split_axis=0, concat_axis=0, tiled=True)


def of_everyone(array, axis):
    return copy_for_each(array, axis).sum(axis=0)


def in_one(arrays, axis):
    ends = [0]
    for a in arrays:
        ends.append(ends[-1] + a.size)
    total = of_everyone(jnp.concatenate([a.ravel() for a in arrays]), axis)
    return tuple((total[b:e].reshape(a.shape) for a, b, e in zip(arrays, ends, ends[1:])))


def shifted(array, axis, by):
    size = lax.axis_size(axis)
    return lax.ppermute(array, axis, [(i, (i + by) % size) for i in range(size)])


def finish_norm(values, total, squares):
    mean_val = total / D
    sq_mean = squares / D
    inv_std = lax.rsqrt(sq_mean - mean_val * mean_val + epsilon)
    return ((values - mean_val[:, None]) * inv_std[:, None], inv_std)


def swapped(rows):
    return rows.reshape(SIDE, SIDE, BLK, -1).swapaxes(0, 1).reshape(rows.shape)


def body(stash_inputs, stash_hidden, grad_in, w_in, b_in, w_out, b_out, ln_gain, plan):
    bwd_slot = plan[0, 0]
    fwd_slot = plan[0, 1]
    fwd_input = lax.dynamic_index_in_dim(stash_inputs[0], fwd_slot, 0, keepdims=False).astype(
        jnp.float32
    )
    bwd_input = lax.dynamic_index_in_dim(stash_inputs[0], bwd_slot, 0, keepdims=False).astype(
        jnp.float32
    )
    bwd_hidden = lax.dynamic_index_in_dim(stash_hidden[0], bwd_slot, 0, keepdims=False)
    upstream = grad_in[0]
    gain_part = ln_gain[0]
    feat_part = w_out.shape[2]
    sums = in_one(
        (
            jnp.sum(fwd_input, axis=1),
            jnp.sum(fwd_input * fwd_input, axis=1),
            jnp.sum(bwd_input, axis=1),
            jnp.sum(bwd_input * bwd_input, axis=1),
        ),
        "col",
    )
    fwd_hat, fwd_inv = finish_norm(fwd_input, sums[0], sums[1])
    bwd_hat, bwd_inv = finish_norm(bwd_input, sums[2], sums[3])
    normed = (fwd_hat * gain_part).astype(jnp.bfloat16)
    normed_all = lax.all_gather(normed, "row", axis=0, tiled=True)
    upstream_all = lax.all_gather(upstream, "row", axis=0, tiled=True)
    lhs = jnp.stack([upstream_all, swapped(upstream_all), normed_all, swapped(normed_all)])
    lhs = lhs.reshape(2, 2, *normed_all.shape)
    saved, terms_f, terms_b = mid(lhs, bwd_hidden, b_in, w_in[0], w_out[0])
    joint_out = lax.psum_scatter(
        jnp.concatenate([terms_f, terms_b], axis=1), "row", scatter_dimension=0, tiled=True
    ).astype(jnp.float32)
    out_sum = joint_out[:, :feat_part]
    norm_grad = joint_out[:, feat_part:]
    output = (out_sum + b_out[0] + fwd_input).astype(jnp.bfloat16)
    scaled = norm_grad * gain_part
    grad_sums = in_one((jnp.sum(scaled, axis=1), jnp.sum(scaled * bwd_hat, axis=1)), "col")
    first_mean = grad_sums[0] / D
    second_mean = grad_sums[1] / D
    in_grad = upstream.astype(jnp.float32) + bwd_inv[:, None] * (
        scaled - first_mean[:, None] - bwd_hat * second_mean[:, None]
    )
    act_recv = shifted(output, "section", 1)
    grad_recv = shifted(in_grad.astype(jnp.bfloat16), "section", -1)
    return (act_recv[None], grad_recv[None], saved[None])


def solution(mesh):
    in_specs = (
        P("section", None, "row", "col"),
        P("section", None, "col", "row"),
        P("section", "row", "col"),
        P("section", "col", "row"),
        P("section", "row"),
        P("section", "row", "col"),
        P("section", "col"),
        P("section", "col"),
        P("section", None),
    )
    out_specs = (P("section", "row", "col"), P("section", "row", "col"), P("section", "col", "row"))
    return jax.shard_map(body, mesh=mesh, in_specs=in_specs, out_specs=out_specs, check_vma=False)
```

```python
import jax
import jax.numpy as jnp
from jax import lax
from jax.experimental import pallas as pl
from jax.experimental.pallas import tpu as pltpu
from jax.sharding import PartitionSpec as P

D = 12288
FT = 256
SIDE = 4
SLOTS = 8
SENDS = 4
BLK = 32

epsilon = 1e-05
root_coef = 0.7978845608028654
cubic_coef = 0.044715

RB1, D1, L1, RB2, D2, L2, A1, AR1, A2, AR2 = range(10)
KINDS = 10


def gelu_value(values):
    inner = root_coef * (values + cubic_coef * values * values * values)
    return 0.5 * values * (1.0 + jnp.tanh(inner))


def gelu_slope(values):
    inner = root_coef * (values + cubic_coef * values * values * values)
    tangent = jnp.tanh(inner)
    return 0.5 * (1.0 + tangent) + 0.5 * values * (1.0 - tangent * tangent) * root_coef * (
        1.0 + 3.0 * cubic_coef * values * values
    )


def dot_nn(a, b):
    return jnp.dot(a, b, preferred_element_type=jnp.float32)


def dot_nt(a, b):
    return lax.dot_general(a, b, (((1,), (1,)), ((), ())), preferred_element_type=jnp.float32)


class Copy:
    def __init__(self, *args):
        self.args = args

    def make(self):
        src, dst, send, recv, dev = self.args
        return pltpu.make_async_remote_copy(
            src_ref=src,
            dst_ref=dst,
            send_sem=send,
            recv_sem=recv,
            device_id=dev,
            device_id_type=pl.DeviceIdType.MESH,
        )

    def start(self):
        self.make().start()

    def wait_recv(self):
        self.make().wait_recv()

    def wait_recv_into(self, dst):
        src, _, send, recv, dev = self.args
        Copy(dst, dst, send, recv, dev).wait_recv()

    def wait_send(self):
        self.make().wait_send()


def step_kernel(
    plan,
    grad,
    gain,
    b_in,
    b_out,
    stash_x,
    stash_h,
    w_in,
    w_out,
    act_recv,
    grad_recv,
    saved,
    lhs,
    xs,
    stash,
    stat_src,
    stat_in,
    stats,
    pair_src,
    pair_in,
    relay_in,
    own_sum,
    far_src,
    far_in,
    sect_src,
    sect_in,
    win_s,
    wout_s,
    parts,
    rb1,
    lr1,
    quart,
    rb2,
    lr2,
    gath,
    acc,
    send_sem,
    recv_sem,
    win_sem,
    wout_sem,
    load_sem,
    side_send,
    side_recv,
):
    n_pair = win_s.shape[0] // 2
    ft = win_s.shape[2]
    units = 2 * n_pair
    f32, bf16 = jnp.float32, jnp.bfloat16
    col = lax.axis_index("col")
    pos = (col // SIDE, lax.rem(col, SIDE))

    def at_x(by):
        return {"col": lax.rem(pos[0] + by + SIDE, SIDE) * SIDE + pos[1]}

    def at_z(by):
        return {"col": pos[0] * SIDE + lax.rem(pos[1] + by + SIDE, SIDE)}

    hops = (at_x, at_z)

    def win_copy(t):
        return pltpu.make_async_copy(
            w_in.at[0, :, pl.ds(pl.multiple_of(t * ft, ft), ft)], win_s.at[t], win_sem.at[t]
        )

    def wout_copy(t):
        return pltpu.make_async_copy(
            w_out.at[0, pl.ds(pl.multiple_of(t * ft, ft), ft), :], wout_s.at[t], wout_sem.at[t]
        )

    rows = SIDE * BLK
    feat = win_s.shape[1]
    row = lax.axis_index("row")
    high, core = row // 2, lax.rem(row, 2)
    section = lax.axis_index("section")
    mate = {"row": high * 2 + 1 - core}
    far = {"row": (1 - high) * 2 + core}
    next_same = {"section": 1 - section, "row": row}
    next_far = {"section": 1 - section, "row": (1 - high) * 2 + core}
    everyone = [at_x(by) for by in (1, 2, 3)] + [at_z(by) for by in (1, 2, 3)]
    everyone += [mate, far, next_same, next_far]

    def side(i, src, dst, dev):
        return Copy(src, dst, side_send.at[i], side_recv.at[i], dev)

    loads = [
        pltpu.make_async_copy(stash_x.at[0], xs, load_sem.at[0]),
        pltpu.make_async_copy(stash_h.at[0], stash, load_sem.at[1]),
    ]
    loads[0].start()

    @pl.loop(0, 2 * n_pair)
    def _(t):
        wout_copy(t).start()

    loads[1].start()

    @pl.loop(0, 2 * n_pair)
    def _(t):
        win_copy(t).start()

    barrier = pltpu.get_barrier_semaphore()
    for dev in everyone:
        pl.semaphore_signal(barrier, inc=1, device_id=dev, device_id_type=pl.DeviceIdType.MESH)
    pl.semaphore_wait(barrier, len(everyone))

    def row_block(high_of, core_of):
        return pl.ds(pl.multiple_of((high_of * 2 + core_of) * rows, rows), rows)

    half = rows // 2
    mine, far_rows = row_block(high, core), row_block(1 - high, core)
    grads = lhs.at[0, 0]

    def half_of(block_high, n):
        return pl.ds(pl.multiple_of((block_high * 2 + core) * rows + n * half, half), half)

    to_mate = side(0, grad.at[0], grads.at[mine], mate)
    out_hops = [
        side(1 + n, grad.at[0, pl.ds(n * half, half)], relay_in.at[n], (next_same, next_far)[n])
        for n in (0, 1)
    ]
    on_hops = [
        side(3 + n, relay_in.at[n], grads.at[half_of(pass_high, n)], (next_far, next_same)[n])
        for n, pass_high in ((0, high), (1, 1 - high))
    ]
    far_to_mate = [
        side(5 + n, grads.at[half_of(1 - high, n)], grads.at[half_of(1 - high, n)], mate)
        for n in (0, 1)
    ]
    for c in out_hops + [to_mate]:
        c.start()
    lhs[0, 0, mine] = grad[0]
    for n in (0, 1):
        out_hops[n].wait_recv()
        on_hops[n].start()

    def pack(columns):
        lane = lax.broadcasted_iota(jnp.int32, (rows, rows), 1)
        grid = jnp.zeros((rows, rows), f32)
        for i, c in enumerate(columns):
            grid = jnp.where(lane == i, c, grid)
        return grid.T[:8]

    def unpack(packed):
        return jnp.concatenate([packed] * (rows // 8), axis=0).T

    def stat_copies(n, axis):
        hop = hops[axis]
        first = 8 + (2 * n + axis) * 3
        return [
            side(first + j - 1, stat_src.at[n, axis], stat_in.at[n, axis, j - 1], hop(j))
            for j in (1, 2, 3)
        ]

    def stat_send(n, axis, value):
        stat_src[n, axis] = value
        for c in stat_copies(n, axis):
            c.start()

    def stat_total(n, axis):
        copies = stat_copies(n, axis)
        for c in copies:
            c.wait_recv()
        total = stat_src[n, axis]
        for j in (0, 1, 2):
            total = total + stat_in[n, axis, j]
        for c in copies:
            c.wait_send()
        return total

    def row_sum(v):
        return jnp.sum(v, axis=1, keepdims=True)

    loads[0].wait()
    fwd_input = xs[plan[0, 1]].astype(f32)
    bwd_input = xs[plan[0, 0]].astype(f32)
    stat_send(
        0,
        0,
        pack(
            [
                row_sum(fwd_input),
                row_sum(fwd_input * fwd_input),
                row_sum(bwd_input),
                row_sum(bwd_input * bwd_input),
            ]
        ),
    )
    loads[1].wait()

    def swap_rows(k):
        @pl.loop(0, SIDE * SIDE)
        def _(b):
            x, z = b // SIDE, lax.rem(b, SIDE)
            lhs[k, 1, pl.ds(pl.multiple_of((z * SIDE + x) * BLK, BLK), BLK)] = lhs[
                k, 0, pl.ds(pl.multiple_of(b * BLK, BLK), BLK)
            ]

    for n in (0, 1):
        on_hops[n].wait_recv_into(grads.at[half_of(1 - high, n)])
        far_to_mate[n].start()
    to_mate.wait_recv()
    for n in (0, 1):
        far_to_mate[n].wait_recv()
    swap_rows(0)
    for c in out_hops + on_hops + far_to_mate + [to_mate]:
        c.wait_send()

    def ring(q, phase):
        axis = (q + phase) % 2
        return pos[axis], hops[axis]

    def wrap(v):
        return lax.rem(v + SIDE, SIDE)

    def copy(kind, q, u, d, src, dst, hop):
        return Copy(
            src,
            dst,
            send_sem.at[kind, q, lax.rem(u, SENDS), d],
            recv_sem.at[kind, q, lax.rem(u, SLOTS), d],
            hop(1 if d == 0 else -1),
        )

    def span(i, size, lo, n):
        return pl.ds(pl.multiple_of(i * size + lo, n), n)

    def scatter_copies(buf, back, side, size, kinds, me, hop, q, u):
        half = size // 2
        s = lax.rem(u, SLOTS)
        far, nxt, prv = wrap(me + 2), wrap(me + 1), wrap(me - 1)
        src = buf.at[q, s]
        relay = [
            copy(kinds[0], q, u, 0, src.at[span(far, size, 0, half)], back.at[q, s, 0], hop),
            copy(kinds[0], q, u, 1, src.at[span(far, size, half, half)], back.at[q, s, 1], hop),
        ]
        direct = [
            copy(kinds[1], q, u, 0, src.at[span(nxt, size, half, half)],
                 side.at[q, s, 0, pl.ds(half, half)], hop),
            copy(kinds[1], q, u, 1, src.at[span(prv, size, 0, half)],
                 side.at[q, s, 1, pl.ds(0, half)], hop),
        ]
        late = [
            copy(kinds[2], q, u, 0, src.at[span(nxt, size, 0, half)],
                 side.at[q, s, 0, pl.ds(0, half)], hop),
            copy(kinds[2], q, u, 1, src.at[span(prv, size, half, half)],
                 side.at[q, s, 1, pl.ds(half, half)], hop),
        ]
        return relay, direct, late

    def relay_step(buf, back, size, copies, me, q, u):
        relay, direct, late = copies
        half = size // 2
        s = lax.rem(u, SLOTS)
        for d, (chunk, lo) in enumerate(((wrap(me + 1), 0), (wrap(me - 1), half))):
            relay[d].wait_recv()
            rows = span(chunk, size, lo, half)
            buf[q, s, rows] = (
                buf[q, s, rows].astype(f32) + back[q, s, d].astype(f32)
            ).astype(bf16)
            late[d].start()
        for c in relay + direct:
            c.wait_send()

    big, small = SIDE * BLK, BLK

    def rs1(q, u):
        me, hop = ring(q, 0)
        return scatter_copies(parts, rb1, lr1, big, (RB1, D1, L1), me, hop, q, u)

    def rs2(q, u):
        me, hop = ring(q, 1)
        return scatter_copies(quart, rb2, lr2, small, (RB2, D2, L2), me, hop, q, u)

    def s0(u, q):
        s = lax.rem(u, SLOTS)

        @pl.when(u < n_pair)
        def _():
            t = 2 * u + q
            wout_copy(t).wait()
            parts[q, s] = dot_nt(lhs[0, q], wout_s[t]).astype(bf16)

        @pl.when(u >= n_pair)
        def _():
            t = 2 * (u - n_pair) + q
            parts[q, s] = dot_nn(lhs[1, q], win_s[t]).astype(bf16)

        relay, direct, _ = rs1(q, u)
        for c in relay + direct:
            c.start()

    def s1(u, q):
        me, _ = ring(q, 0)
        relay_step(parts, rb1, big, rs1(q, u), me, q, u)

    def s2(u, q):
        me, _ = ring(q, 0)
        s = lax.rem(u, SLOTS)
        _, direct, late = rs1(q, u)
        for c in direct + late:
            c.wait_recv()
        quart[q, s] = (
            parts[q, s, span(me, big, 0, big)].astype(f32)
            + lr1[q, s, 0].astype(f32)
            + lr1[q, s, 1].astype(f32)
        ).astype(bf16)
        relay, direct, _ = rs2(q, u)
        for c in relay + direct:
            c.start()
        for c in late:
            c.wait_send()

    def s3(u, q):
        me, _ = ring(q, 1)
        relay_step(quart, rb2, small, rs2(q, u), me, q, u)

    def gather1(q, u):
        me1, _ = ring(q, 0)
        me, hop = ring(q, 1)
        g = gath.at[q, lax.rem(u, SLOTS), me1]
        half = BLK // 2
        own = [copy(A1, q, u, d, g.at[me], g.at[me], hop) for d in (0, 1)]
        on = []
        for d, (b, lo) in enumerate(((wrap(me - 1), 0), (wrap(me + 1), half))):
            r = g.at[b, pl.ds(lo, half)]
            on.append(copy(AR1, q, u, d, r, r, hop))
        return own, on

    def gather2(q, u):
        me, hop = ring(q, 0)
        g = gath.at[q, lax.rem(u, SLOTS)]
        own = [copy(A2, q, u, d, g.at[me], g.at[me], hop) for d in (0, 1)]
        on = []
        for d, (b, lo) in enumerate(((wrap(me - 1), 0), (wrap(me + 1), SIDE // 2))):
            r = g.at[b, pl.ds(lo, SIDE // 2)]
            on.append(copy(AR2, q, u, d, r, r, hop))
        return own, on

    def s4(u, q):
        me1, _ = ring(q, 0)
        me2, _ = ring(q, 1)
        s = lax.rem(u, SLOTS)
        _, direct, late = rs2(q, u)
        for c in direct + late:
            c.wait_recv()
        h = (
            quart[q, s, span(me2, small, 0, small)].astype(f32)
            + lr2[q, s, 0].astype(f32)
            + lr2[q, s, 1].astype(f32)
        )

        @pl.when(u < n_pair)
        def _():
            t = 2 * u + q
            cols = pl.ds(pl.multiple_of(t * ft, ft), ft)
            slope = gelu_slope(stash[plan[0, 0], :, cols].astype(f32))
            gath[q, s, me1, me2] = (h * slope).astype(bf16)

        @pl.when(u >= n_pair)
        def _():
            t = 2 * (u - n_pair) + q
            cols = pl.ds(pl.multiple_of(t * ft, ft), ft)
            hidden = h + b_in[:, cols]
            saved[0, :, cols] = hidden.astype(bf16)
            gath[q, s, me1, me2] = gelu_value(hidden).astype(bf16)

        own, _ = gather1(q, u)
        for c in own:
            c.start()
        for c in late:
            c.wait_send()

    def pass_on(own, on):
        for d in (0, 1):
            own[d].wait_recv()
            on[d].start()
        for c in own:
            c.wait_send()

    def s5(u, q):
        pass_on(*gather1(q, u))

    def s6(u, q):
        _, on = gather1(q, u)
        for c in on:
            c.wait_recv()
        own, _ = gather2(q, u)
        for c in own:
            c.start()
        for c in on:
            c.wait_send()

    def s7(u, q):
        pass_on(*gather2(q, u))

    def s8(u, q):
        s = lax.rem(u, SLOTS)
        _, on = gather2(q, u)
        for c in on:
            c.wait_recv()
        for c in on:
            c.wait_send()
        rows = SIDE * SIDE * BLK
        piece = gath[q, s].reshape(rows, ft)

        def add(kind, first, value):
            @pl.when(first)
            def _():
                acc[kind, q] = value

            @pl.when(jnp.logical_not(first))
            def _():
                acc[kind, q] += value

        @pl.when(u < n_pair)
        def _():
            t = 2 * u + q
            win_copy(t).wait()
            add(0, u == 0, dot_nt(piece, win_s[t]))

        @pl.when(u >= n_pair)
        def _():
            t = 2 * (u - n_pair) + q
            add(1, u == n_pair, dot_nn(piece, wout_s[t]))

    stages = (s0, s1, s2, s3, s4, s5, s6, s7, s8)
    normed_rows = lhs.at[1, 0]
    base = 20
    normed_to_mate = side(base, normed_rows.at[mine], normed_rows.at[mine], mate)
    normed_to_far = side(base + 1, normed_rows.at[mine], normed_rows.at[mine], far)
    normed_on = side(base + 2, normed_rows.at[far_rows], normed_rows.at[far_rows], mate)
    pair_sum = [side(base + 3 + k, pair_src.at[k], pair_in.at[k], mate) for k in (0, 1)]
    far_sum = side(base + 5, far_src, far_in, far)
    grad_on = side(base + 6, sect_src.at[0], sect_in.at[0], next_same)
    act_on = [
        side(base + 7, sect_src.at[1], sect_in.at[1], next_same),
        side(base + 8, sect_src.at[2], sect_in.at[2], next_far),
    ]

    def total_rows(k, high_of, core_of):
        r = high_of * 2 + core_of
        pieces = []
        for z in range(SIDE):
            own = pl.ds(pl.multiple_of((r * SIDE + z) * BLK, BLK), BLK)
            swap = pl.ds(pl.multiple_of((z * SIDE + r) * BLK, BLK), BLK)
            pieces.append(acc[k, 0, own] + acc[k, 1, swap])
        return jnp.concatenate(pieces, axis=0)

    def send_pair(k):
        for h in (0, 1):
            pair_src[k, h] = total_rows(k, h, 1 - core).astype(bf16)
        pair_sum[k].start()

    def chip_rows(k, high_of):
        return total_rows(k, high_of, core) + pair_in[k, high_of].astype(f32)

    def norm_stats():
        stat_send(0, 1, stat_total(0, 0))

    def normalize():
        total = unpack(stat_total(0, 1)) / D
        mean_f, mean_b = total[:, 0:1], total[:, 2:3]
        inv_f = lax.rsqrt(total[:, 1:2] - mean_f * mean_f + epsilon)
        inv_b = lax.rsqrt(total[:, 3:4] - mean_b * mean_b + epsilon)
        stats[0] = jnp.broadcast_to(mean_b, (rows, rows))
        stats[1] = jnp.broadcast_to(inv_b, (rows, rows))
        values = xs[plan[0, 1]].astype(f32)
        lhs[1, 0, mine] = ((values - mean_f) * inv_f * gain[...]).astype(bf16)
        normed_to_mate.start()
        normed_to_far.start()

    def normed_forward():
        normed_to_far.wait_recv_into(normed_rows.at[far_rows])
        normed_on.start()

    def normed_done():
        normed_to_mate.wait_recv()
        normed_on.wait_recv()
        swap_rows(1)
        for c in (normed_to_mate, normed_to_far, normed_on):
            c.wait_send()

    def grad_far():
        pair_sum[0].wait_recv()
        own_sum[...] = chip_rows(0, high)
        far_src[...] = chip_rows(0, 1 - high).astype(bf16)
        far_sum.start()
        pair_sum[0].wait_send()

    def hat():
        return (xs[plan[0, 0]].astype(f32) - stats[0, :, 0:1]) * stats[1, :, 0:1]

    def grad_stats():
        far_sum.wait_recv()
        scaled = (own_sum[...] + far_in[...].astype(f32)) * gain[...]
        own_sum[...] = scaled
        stat_send(1, 0, pack([row_sum(scaled), row_sum(scaled * hat())]))
        far_sum.wait_send()

    def grad_stats_more():
        stat_send(1, 1, stat_total(1, 0))

    def grad_out():
        total = unpack(stat_total(1, 1)) / D
        in_grad = grad[0].astype(f32) + stats[1, :, 0:1] * (
            own_sum[...] - total[:, 0:1] - hat() * total[:, 1:2]
        )
        sect_src[0] = in_grad.astype(bf16)
        grad_on.start()

    last = n_pair + len(stages) - 1
    jobs = (
        (2, norm_stats),
        (4, normalize),
        (7, normed_forward),
        (9, normed_done),
        (last, lambda: send_pair(0)),
        (last + 1, grad_far),
        (last + 4, grad_stats),
        (last + 6, grad_stats_more),
        (last + 8, grad_out),
    )

    @pl.loop(0, units + len(stages) - 1)
    def _(step):
        for k, stage in enumerate(stages):
            u = step - k

            @pl.when(jnp.logical_and(u >= 0, u < units))
            def _():
                for q in (0, 1):
                    stage(u, q)

            if k == 0:
                for at, job in jobs:
                    pl.when(step == at)(job)

    send_pair(1)
    grad_on.wait_recv()
    grad_recv[0] = sect_in[0]
    residual = xs[plan[0, 1]].astype(f32) + b_out[...]
    pair_sum[1].wait_recv()
    sect_src[1] = (chip_rows(1, high) + residual).astype(bf16)
    act_on[0].start()
    sect_src[2] = chip_rows(1, 1 - high).astype(bf16)
    act_on[1].start()
    for c in act_on:
        c.wait_recv()
    act_recv[0] = (sect_in[1].astype(f32) + sect_in[2].astype(f32)).astype(bf16)
    for c in act_on + [pair_sum[1], grad_on]:
        c.wait_send()


def body(stash_inputs, stash_hidden, grad_in, w_in, b_in, w_out, b_out, ln_gain, plan, ft=FT):
    _, feat, hid = w_in.shape
    slots = stash_inputs.shape[1]
    tiles = hid // ft
    rows, mine = SIDE * SIDE * BLK, SIDE * BLK
    bf16, f32 = jnp.bfloat16, jnp.float32
    vmem, anyw = pl.BlockSpec(memory_space=pltpu.VMEM), pl.BlockSpec(memory_space=pl.ANY)
    return pl.pallas_call(
        step_kernel,
        out_shape=(
            jax.ShapeDtypeStruct((1, mine, feat), bf16),
            jax.ShapeDtypeStruct((1, mine, feat), bf16),
            jax.ShapeDtypeStruct((1, BLK, hid), bf16),
        ),
        in_specs=[pl.BlockSpec(memory_space=pltpu.SMEM), vmem, vmem, vmem, vmem] + [anyw] * 4,
        out_specs=(vmem, vmem, vmem),
        scratch_shapes=[
            pltpu.VMEM((2, 2, rows, feat), bf16),
            pltpu.VMEM((slots, mine, feat), bf16),
            pltpu.VMEM((slots, BLK, hid), bf16),
            pltpu.VMEM((2, 2, 8, mine), f32),
            pltpu.VMEM((2, 2, 3, 8, mine), f32),
            pltpu.VMEM((2, mine, mine), f32),
            pltpu.VMEM((2, 2, mine, feat), bf16),
            pltpu.VMEM((2, 2, mine, feat), bf16),
            pltpu.VMEM((2, mine // 2, feat), bf16),
            pltpu.VMEM((mine, feat), f32),
            pltpu.VMEM((mine, feat), bf16),
            pltpu.VMEM((mine, feat), bf16),
            pltpu.VMEM((3, mine, feat), bf16),
            pltpu.VMEM((3, mine, feat), bf16),
            pltpu.VMEM((tiles, feat, ft), bf16),
            pltpu.VMEM((tiles, ft, feat), bf16),
            pltpu.VMEM((2, SLOTS, rows, ft), bf16),
            pltpu.VMEM((2, SLOTS, 2, 2 * BLK, ft), bf16),
            pltpu.VMEM((2, SLOTS, 2, 4 * BLK, ft), bf16),
            pltpu.VMEM((2, SLOTS, 4 * BLK, ft), bf16),
            pltpu.VMEM((2, SLOTS, 2, BLK // 2, ft), bf16),
            pltpu.VMEM((2, SLOTS, 2, BLK, ft), bf16),
            pltpu.VMEM((2, SLOTS, SIDE, SIDE, BLK, ft), bf16),
            pltpu.VMEM((2, 2, rows, feat), f32),
            pltpu.SemaphoreType.DMA((KINDS, 2, SENDS, 2)),
            pltpu.SemaphoreType.DMA((KINDS, 2, SLOTS, 2)),
            pltpu.SemaphoreType.DMA((tiles,)),
            pltpu.SemaphoreType.DMA((tiles,)),
            pltpu.SemaphoreType.DMA((2,)),
            pltpu.SemaphoreType.DMA((32,)),
            pltpu.SemaphoreType.DMA((32,)),
        ],
        compiler_params=pltpu.CompilerParams(
            collective_id=0, has_side_effects=True, vmem_limit_bytes=67043328
        ),
        name="section_step",
    )(plan, grad_in, ln_gain, b_in, b_out, stash_inputs, stash_hidden, w_in, w_out)


def solution(mesh):
    in_specs = (
        P("section", None, "row", "col"),
        P("section", None, "col", "row"),
        P("section", "row", "col"),
        P("section", "col", "row"),
        P("section", "row"),
        P("section", "row", "col"),
        P("section", "col"),
        P("section", "col"),
        P("section", None),
    )
    out_specs = (P("section", "row", "col"), P("section", "row", "col"), P("section", "col", "row"))
    return jax.shard_map(body, mesh=mesh, in_specs=in_specs, out_specs=out_specs, check_vma=False)
```

```python
import jax
import jax.numpy as jnp
from jax import lax
from jax.experimental import pallas as pl
from jax.experimental.pallas import tpu as pltpu
from jax.sharding import PartitionSpec as P

D = 12288
FT = 512
SIDE = 4
SLOTS = 8
LOCAL = 4
BLK = 32
LATE_STAGE = 8
PIECES = 8
PARTS = 3
FRONT = 32

epsilon = 1e-05
root_coef = 0.7978845608028654
cubic_coef = 0.044715

RB1, LR1, RB2, LR2, A1, AR1, A2, AR2 = range(8)
SEND_RING = (0, 0, 1, 1, 2, 2, 3, 3)


def gelu_value(values):
    inner = root_coef * (values + cubic_coef * values * values * values)
    return 0.5 * values * (1.0 + jnp.tanh(inner))


def gelu_slope(values):
    inner = root_coef * (values + cubic_coef * values * values * values)
    tangent = jnp.tanh(inner)
    return 0.5 * (1.0 + tangent) + 0.5 * values * (1.0 - tangent * tangent) * root_coef * (
        1.0 + 3.0 * cubic_coef * values * values
    )


def dot_nn(a, b):
    return jnp.dot(a, b, preferred_element_type=jnp.float32)


def dot_nt(a, b):
    return lax.dot_general(a, b, (((1,), (1,)), ((), ())), preferred_element_type=jnp.float32)


class Copy:
    def __init__(self, *args):
        self.args = args

    def make(self):
        src, dst, send, recv, dev = self.args
        return pltpu.make_async_remote_copy(
            src_ref=src,
            dst_ref=dst,
            send_sem=send,
            recv_sem=recv,
            device_id=dev,
            device_id_type=pl.DeviceIdType.MESH,
        )

    def start(self):
        self.make().start()

    def wait_recv(self):
        self.make().wait_recv()

    def wait_recv_into(self, dst):
        src, _, send, recv, dev = self.args
        Copy(dst, dst, send, recv, dev).wait_recv()

    def wait_send(self):
        self.make().wait_send()


def step_kernel(
    plan,
    grad,
    gain,
    b_in,
    b_out,
    stash_x,
    stash_h,
    w_in,
    w_out,
    act_recv,
    grad_recv,
    saved,
    lhs,
    xs,
    stash,
    stat_src,
    stat_in,
    stats,
    pair_src,
    pair_in,
    relay_in,
    own_sum,
    far_src,
    far_in,
    sect_src,
    sect_in,
    win_s,
    wout_s,
    parts,
    rb1,
    lr1,
    quart,
    rb2,
    lr2,
    gath,
    acc,
    send_sem,
    recv_sem,
    win_sem,
    wout_sem,
    load_sem,
    side_send,
    side_recv,
):
    n_pair = win_s.shape[0] // 2
    ft = win_s.shape[2]
    units = 2 * n_pair
    f32, bf16 = jnp.float32, jnp.bfloat16
    col = lax.axis_index("col")
    pos = (col // SIDE, lax.rem(col, SIDE))

    def wrap(v):
        return jnp.bitwise_and(v + SIDE, SIDE - 1)

    along = (
        [{"col": wrap(pos[0] + by) * SIDE + pos[1]} for by in (1, 2, 3)],
        [{"col": pos[0] * SIDE + wrap(pos[1] + by)} for by in (1, 2, 3)],
    )
    hops = tuple((ring[0], ring[2]) for ring in along)
    places = tuple((p, wrap(p + 1), wrap(p + 2), wrap(p + 3)) for p in pos)

    def slot(u):
        return jnp.bitwise_and(u, SLOTS - 1)

    def local(u):
        return jnp.bitwise_and(u, LOCAL - 1)

    def win_copy(t):
        return pltpu.make_async_copy(
            w_in.at[0, :, pl.ds(pl.multiple_of(t * ft, ft), ft)], win_s.at[t], win_sem.at[t]
        )

    def wout_copy(t):
        return pltpu.make_async_copy(
            w_out.at[0, pl.ds(pl.multiple_of(t * ft, ft), ft), :], wout_s.at[t], wout_sem.at[t]
        )

    rows = SIDE * BLK
    feat = win_s.shape[1]
    row = lax.axis_index("row")
    high, core = row // 2, lax.rem(row, 2)
    section = lax.axis_index("section")
    mate = {"row": high * 2 + 1 - core}
    far = {"row": (1 - high) * 2 + core}
    next_same = {"section": 1 - section, "row": row}
    next_far = {"section": 1 - section, "row": (1 - high) * 2 + core}
    everyone = [*along[0], *along[1], mate, far, next_same, next_far]

    def side(i, src, dst, dev):
        return Copy(src, dst, side_send.at[i], side_recv.at[i], dev)

    loads = [
        pltpu.make_async_copy(stash_x.at[0], xs, load_sem.at[0]),
        pltpu.make_async_copy(stash_h.at[0], stash, load_sem.at[1]),
    ]
    loads[0].start()

    @pl.loop(0, 2 * n_pair)
    def _(t):
        wout_copy(t).start()

    loads[1].start()

    @pl.loop(0, 2 * n_pair)
    def _(t):
        win_copy(t).start()

    barrier = pltpu.get_barrier_semaphore()
    for dev in everyone:
        pl.semaphore_signal(barrier, inc=1, device_id=dev, device_id_type=pl.DeviceIdType.MESH)
    pl.semaphore_wait(barrier, len(everyone))

    def row_block(high_of, core_of):
        return pl.ds(pl.multiple_of((high_of * 2 + core_of) * rows, rows), rows)

    piece = rows // PIECES
    mine, far_rows = row_block(high, core), row_block(1 - high, core)
    grads = lhs.at[0, 0]

    def piece_of(block_high, n):
        return pl.ds(pl.multiple_of((block_high * 2 + core) * rows + n * piece, piece), piece)

    by_way = (next_same, next_far)
    to_mate = side(0, grad.at[0], grads.at[mine], mate)
    out_hops = [
        side(FRONT + n, grad.at[0, pl.ds(n * piece, piece)], relay_in.at[n], by_way[n % 2])
        for n in range(PIECES)
    ]
    on_hops = [
        side(
            FRONT + PIECES + n,
            relay_in.at[n],
            grads.at[piece_of((high, 1 - high)[n % 2], n)],
            by_way[1 - n % 2],
        )
        for n in range(PIECES)
    ]
    far_to_mate = [
        side(
            FRONT + 2 * PIECES + n,
            grads.at[piece_of(1 - high, n)],
            grads.at[piece_of(1 - high, n)],
            mate,
        )
        for n in range(PIECES)
    ]
    for c in out_hops + [to_mate]:
        c.start()
    lhs[0, 0, mine] = grad[0]
    for n in range(PIECES):
        out_hops[n].wait_recv()
        on_hops[n].start()

    def pack(columns):
        lane = lax.broadcasted_iota(jnp.int32, (rows, rows), 1)
        grid = jnp.zeros((rows, rows), f32)
        for i, c in enumerate(columns):
            grid = jnp.where(lane == i, c, grid)
        return grid.T[:8]

    def unpack(packed):
        return jnp.concatenate([packed] * (rows // 8), axis=0).T

    def stat_copies(n, axis):
        first = 8 + (2 * n + axis) * 3
        return [
            side(first + j - 1, stat_src.at[n, axis], stat_in.at[n, axis, j - 1], along[axis][j - 1])
            for j in (1, 2, 3)
        ]

    def stat_send(n, axis, value):
        stat_src[n, axis] = value
        for c in stat_copies(n, axis):
            c.start()

    def stat_total(n, axis):
        copies = stat_copies(n, axis)
        for c in copies:
            c.wait_recv()
        total = stat_src[n, axis]
        for j in (0, 1, 2):
            total = total + stat_in[n, axis, j]
        for c in copies:
            c.wait_send()
        return total

    def row_sum(v):
        return jnp.sum(v, axis=1, keepdims=True)

    loads[0].wait()
    fwd_input = xs[plan[0, 1]].astype(f32)
    bwd_input = xs[plan[0, 0]].astype(f32)
    stat_send(
        0,
        0,
        pack(
            [
                row_sum(fwd_input),
                row_sum(fwd_input * fwd_input),
                row_sum(bwd_input),
                row_sum(bwd_input * bwd_input),
            ]
        ),
    )
    loads[1].wait()

    def swap_rows(k, r):
        for z in range(SIDE):
            lhs[k, 1, pl.ds(pl.multiple_of((z * SIDE + r) * BLK, BLK), BLK)] = lhs[
                k, 0, pl.ds(pl.multiple_of((r * SIDE + z) * BLK, BLK), BLK)
            ]

    far_row = (1 - high) * 2 + core
    mate_row, far_mate_row = high * 2 + 1 - core, (1 - high) * 2 + 1 - core
    swap_rows(0, row)
    for n in range(PIECES):
        on_hops[n].wait_recv_into(grads.at[piece_of(1 - high, n)])
        far_to_mate[n].start()
    to_mate.wait_recv()
    swap_rows(0, mate_row)
    swap_rows(0, far_row)
    for n in range(PIECES):
        far_to_mate[n].wait_recv()
    swap_rows(0, far_mate_row)
    for c in out_hops + on_hops + far_to_mate + [to_mate]:
        c.wait_send()

    def ring(q, phase):
        axis = (q + phase) % 2
        return places[axis], hops[axis]

    def copy(kind, q, u, d, src, dst, hop):
        return Copy(
            src,
            dst,
            send_sem.at[SEND_RING[kind], q, local(u)],
            recv_sem.at[kind, q, slot(u)],
            hop[d],
        )

    def arrived(kind, q, u, ref):
        Copy(ref, ref, send_sem.at[0, q, 0], recv_sem.at[kind, q, slot(u)], hops[0][0]).wait_recv()

    def all_sent(ring_no, q, u, ref):
        Copy(ref, ref, send_sem.at[ring_no, q, local(u)], recv_sem.at[0, q, 0], hops[0][0]).wait_send()

    def span(i, size, lo, n):
        return pl.ds(pl.multiple_of(i * size + lo, n), n)

    def scatter_first(buf, back, side_buf, size, kinds, place, hop, q, u):
        half = size // 2
        me, nxt, far_one, prv = place
        src, s = buf.at[q, local(u)], slot(u)
        copy(kinds[0], q, u, 0, src.at[span(far_one, size, 0, half)], back.at[q, s, 0], hop).start()
        copy(kinds[0], q, u, 1, src.at[span(far_one, size, half, half)], back.at[q, s, 1], hop).start()
        copy(kinds[1], q, u, 0, src.at[span(nxt, size, half, half)],
             side_buf.at[q, s, 0, pl.ds(half, half)], hop).start()
        copy(kinds[1], q, u, 1, src.at[span(prv, size, 0, half)],
             side_buf.at[q, s, 1, pl.ds(0, half)], hop).start()

    def scatter_relay(buf, back, side_buf, size, kinds, place, hop, q, u):
        half = size // 2
        me, nxt, far_one, prv = place
        l, s = local(u), slot(u)
        arrived(kinds[0], q, u, back.at[q, s])
        for d, (chunk, lo) in enumerate(((nxt, 0), (prv, half))):
            rows = span(chunk, size, lo, half)
            buf[q, l, rows] = (
                buf[q, l, rows].astype(f32) + back[q, s, d].astype(f32)
            ).astype(bf16)
            copy(kinds[1], q, u, d, buf.at[q, l, rows],
                 side_buf.at[q, s, d, pl.ds(lo, half)], hop).start()

    big, small = SIDE * BLK, BLK

    def s0(u, q):
        l = local(u)

        @pl.when(u < n_pair)
        def _():
            t = 2 * u + q
            wout_copy(t).wait()
            parts[q, l] = dot_nt(lhs[0, q], wout_s[t]).astype(bf16)

        @pl.when(u >= n_pair)
        def _():
            t = 2 * (u - n_pair) + q
            if n_pair < LATE_STAGE - 1:
                win_copy(t).wait()
            parts[q, l] = dot_nn(lhs[1, q], win_s[t]).astype(bf16)

        scatter_first(parts, rb1, lr1, big, (RB1, LR1), *ring(q, 0), q, u)

    def s1(u, q):
        scatter_relay(parts, rb1, lr1, big, (RB1, LR1), *ring(q, 0), q, u)

    def s2(u, q):
        place, _ = ring(q, 0)
        l, s = local(u), slot(u)
        arrived(LR1, q, u, lr1.at[q, s])
        quart[q, l] = (
            parts[q, l, span(place[0], big, 0, big)].astype(f32)
            + lr1[q, s, 0].astype(f32)
            + lr1[q, s, 1].astype(f32)
        ).astype(bf16)
        scatter_first(quart, rb2, lr2, small, (RB2, LR2), *ring(q, 1), q, u)
        all_sent(0, q, u, parts.at[q, l, pl.ds(0, 3 * big)])

    def s3(u, q):
        scatter_relay(quart, rb2, lr2, small, (RB2, LR2), *ring(q, 1), q, u)

    def s4(u, q):
        me1 = ring(q, 0)[0][0]
        place, hop = ring(q, 1)
        me2 = place[0]
        l, s = local(u), slot(u)
        arrived(LR2, q, u, lr2.at[q, s])
        h = (
            quart[q, l, span(me2, small, 0, small)].astype(f32)
            + lr2[q, s, 0].astype(f32)
            + lr2[q, s, 1].astype(f32)
        )

        @pl.when(u < n_pair)
        def _():
            t = 2 * u + q
            cols = pl.ds(pl.multiple_of(t * ft, ft), ft)
            slope = gelu_slope(stash[plan[0, 0], :, cols].astype(f32))
            gath[q, s, me1, me2] = (h * slope).astype(bf16)

        @pl.when(u >= n_pair)
        def _():
            t = 2 * (u - n_pair) + q
            cols = pl.ds(pl.multiple_of(t * ft, ft), ft)
            hidden = h + b_in[:, cols]
            saved[0, :, cols] = hidden.astype(bf16)
            gath[q, s, me1, me2] = gelu_value(hidden).astype(bf16)

        g = gath.at[q, s, me1, me2]
        for d in (0, 1):
            copy(A1, q, u, d, g, g, hop).start()
        all_sent(1, q, u, quart.at[q, l, pl.ds(0, 3 * small)])

    def s5(u, q):
        me1 = ring(q, 0)[0][0]
        place, hop = ring(q, 1)
        g = gath.at[q, slot(u), me1]
        arrived(A1, q, u, g.at[pl.ds(0, 2)])
        for d, (b, lo) in enumerate(((place[3], 0), (place[1], BLK // 2))):
            r = g.at[b, pl.ds(lo, BLK // 2)]
            copy(AR1, q, u, d, r, r, hop).start()

    def product(u, q, blocks):
        s = slot(u)

        def add(kind, first, values):
            @pl.when(first)
            def _():
                for b, value in zip(blocks, values):
                    acc[kind, q, span(b, big, 0, big)] = value

            @pl.when(jnp.logical_not(first))
            def _():
                for b, value in zip(blocks, values):
                    acc[kind, q, span(b, big, 0, big)] += value

        pieces = [gath[q, s, b].reshape(big, ft) for b in blocks]

        @pl.when(u < n_pair)
        def _():
            t = 2 * u + q
            add(0, u == 0, [dot_nt(piece, win_s[t]) for piece in pieces])

        @pl.when(u >= n_pair)
        def _():
            t = 2 * (u - n_pair) + q
            add(1, u == n_pair, [dot_nn(piece, wout_s[t]) for piece in pieces])

    def s6(u, q):
        place, hop = ring(q, 0)
        me1 = place[0]
        g = gath.at[q, slot(u)]
        arrived(AR1, q, u, g.at[me1, 0])
        for d in (0, 1):
            copy(A2, q, u, d, g.at[me1], g.at[me1], hop).start()
        if n_pair >= LATE_STAGE - 1:

            @pl.when(u < n_pair)
            def _():
                win_copy(2 * u + q).wait()

        product(u, q, [me1])
        all_sent(2, q, u, g.at[me1, pl.ds(0, 3)])

    def s7(u, q):
        place, hop = ring(q, 0)
        g = gath.at[q, slot(u)]
        arrived(A2, q, u, g.at[pl.ds(0, 2)])
        for d, (b, lo) in enumerate(((place[3], 0), (place[1], SIDE // 2))):
            r = g.at[b, pl.ds(lo, SIDE // 2)]
            copy(AR2, q, u, d, r, r, hop).start()
        product(u, q, [place[1], place[3]])

    def s8(u, q):
        place, _ = ring(q, 0)
        g = gath.at[q, slot(u)]
        arrived(AR2, q, u, g.at[0])
        product(u, q, [place[2]])
        all_sent(3, q, u, g.at[pl.ds(0, 3)])

    stages = (s0, s1, s2, s3, s4, s5, s6, s7, s8)
    normed_rows = lhs.at[1, 0]
    base = 20
    normed_to_mate = side(base, normed_rows.at[mine], normed_rows.at[mine], mate)
    normed_to_far = side(base + 1, normed_rows.at[mine], normed_rows.at[mine], far)
    normed_on = side(base + 2, normed_rows.at[far_rows], normed_rows.at[far_rows], mate)
    pair_sum = side(base + 3, pair_src.at[0], pair_in.at[0], mate)
    far_sum = side(base + 5, far_src, far_in, far)
    grad_on = side(base + 6, sect_src.at[0], sect_in.at[0], next_same)
    wide = feat // PARTS
    cuts = [pl.ds(p * wide, wide) for p in range(PARTS)]
    tail = FRONT + 3 * PIECES
    pair_parts = [
        side(tail + p, pair_src.at[1, :, :, c], pair_in.at[1, :, :, c], mate)
        for p, c in enumerate(cuts)
    ]
    act_parts = [
        [
            side(
                tail + PARTS + 2 * p + n,
                sect_src.at[1 + n, :, c],
                sect_in.at[1 + n, :, c],
                by_way[n],
            )
            for n in (0, 1)
        ]
        for p, c in enumerate(cuts)
    ]

    def total_rows(k, high_of, core_of, cut):
        r = high_of * 2 + core_of
        pieces = []
        for z in range(SIDE):
            own = pl.ds(pl.multiple_of((r * SIDE + z) * BLK, BLK), BLK)
            swap = pl.ds(pl.multiple_of((z * SIDE + r) * BLK, BLK), BLK)
            pieces.append(acc[k, 0, own, cut] + acc[k, 1, swap, cut])
        return jnp.concatenate(pieces, axis=0)

    def pair_part(k, cut):
        for h in (0, 1):
            pair_src[k, h, :, cut] = total_rows(k, h, 1 - core, cut).astype(bf16)

    def chip_rows(k, high_of, cut):
        return total_rows(k, high_of, core, cut) + pair_in[k, high_of, :, cut].astype(f32)

    def grad_pair():
        pair_part(0, slice(None))
        pair_sum.start()

    def norm_stats():
        stat_send(0, 1, stat_total(0, 0))

    def normalize():
        total = unpack(stat_total(0, 1)) / D
        mean_f, mean_b = total[:, 0:1], total[:, 2:3]
        inv_f = lax.rsqrt(total[:, 1:2] - mean_f * mean_f + epsilon)
        inv_b = lax.rsqrt(total[:, 3:4] - mean_b * mean_b + epsilon)
        stats[0] = jnp.broadcast_to(mean_b, (rows, rows))
        stats[1] = jnp.broadcast_to(inv_b, (rows, rows))
        values = xs[plan[0, 1]].astype(f32)
        lhs[1, 0, mine] = ((values - mean_f) * inv_f * gain[...]).astype(bf16)
        normed_to_mate.start()
        normed_to_far.start()

    def normed_forward():
        normed_to_far.wait_recv_into(normed_rows.at[far_rows])
        normed_on.start()

    def normed_done():
        normed_to_mate.wait_recv()
        normed_on.wait_recv()
        for r in (row, mate_row, far_row, far_mate_row):
            swap_rows(1, r)
        for c in (normed_to_mate, normed_to_far, normed_on):
            c.wait_send()

    def grad_far():
        pair_sum.wait_recv()
        own_sum[...] = chip_rows(0, high, slice(None))
        far_src[...] = chip_rows(0, 1 - high, slice(None)).astype(bf16)
        far_sum.start()
        pair_sum.wait_send()

    def hat():
        return (xs[plan[0, 0]].astype(f32) - stats[0, :, 0:1]) * stats[1, :, 0:1]

    def grad_stats():
        far_sum.wait_recv()
        scaled = (own_sum[...] + far_in[...].astype(f32)) * gain[...]
        own_sum[...] = scaled
        stat_send(1, 0, pack([row_sum(scaled), row_sum(scaled * hat())]))
        far_sum.wait_send()

    def grad_stats_more():
        stat_send(1, 1, stat_total(1, 0))

    def grad_out():
        total = unpack(stat_total(1, 1)) / D
        in_grad = grad[0].astype(f32) + stats[1, :, 0:1] * (
            own_sum[...] - total[:, 0:1] - hat() * total[:, 1:2]
        )
        sect_src[0] = in_grad.astype(bf16)
        grad_on.start()

    last = n_pair + len(stages) - 2
    early = (2, 4, 7, 9) if n_pair >= 10 else (1, 2, 4, 5)
    jobs = (
        (early[0], 0, norm_stats),
        (early[1], 0, normalize),
        (early[2], 0, normed_forward),
        (early[3], 0, normed_done),
        (last, 8, grad_pair),
        (last + 1, 3, grad_far),
        (last + 3, 3, grad_stats),
        (last + 4, 0, grad_stats_more),
        (last + 4, 7, grad_out),
    )

    @pl.loop(0, units + len(stages) - 1)
    def _(step):
        for k, stage in enumerate(stages):
            u = step - k

            @pl.when(jnp.logical_and(u >= 0, u < units))
            def _():
                for q in (0, 1):
                    stage(u, q)

            for at, after, job in jobs:
                if after == k:
                    pl.when(step == at)(job)

    for p, c in enumerate(cuts):
        pair_part(1, c)
        pair_parts[p].start()
    for p, c in enumerate(cuts):
        pair_parts[p].wait_recv()
        sect_src[2, :, c] = chip_rows(1, 1 - high, c).astype(bf16)
        act_parts[p][1].start()
        residual = xs[plan[0, 1], :, c].astype(f32) + b_out[:, c]
        sect_src[1, :, c] = (chip_rows(1, high, c) + residual).astype(bf16)
        act_parts[p][0].start()
    grad_on.wait_recv()
    grad_recv[0] = sect_in[0]
    for p, c in enumerate(cuts):
        for n in (0, 1):
            act_parts[p][n].wait_recv()
        act_recv[0, :, c] = (
            sect_in[1, :, c].astype(f32) + sect_in[2, :, c].astype(f32)
        ).astype(bf16)
    for c in pair_parts + act_parts[0] + act_parts[1] + act_parts[2] + [grad_on]:
        c.wait_send()


def store_kernel(*refs):
    n = (len(refs) - 2) // 3
    ins, outs, held = refs[:n], refs[n : 2 * n], refs[2 * n : 3 * n]
    get = [pltpu.make_async_copy(ins[i], held[i], refs[-2].at[i]) for i in range(n)]
    put = [pltpu.make_async_copy(held[i], outs[i], refs[-1].at[i]) for i in range(n)]
    for c in get:
        c.start()
    for i in range(n):
        get[i].wait()
        put[i].start()
    for c in put:
        c.wait()


def body(stash_inputs, stash_hidden, grad_in, w_in, b_in, w_out, b_out, ln_gain, plan, ft=FT):
    _, feat, hid = w_in.shape
    slots = stash_inputs.shape[1]
    tiles = hid // ft
    rows, mine = SIDE * SIDE * BLK, SIDE * BLK
    bf16, f32 = jnp.bfloat16, jnp.float32
    vmem, anyw = pl.BlockSpec(memory_space=pltpu.VMEM), pl.BlockSpec(memory_space=pl.ANY)
    results = pl.pallas_call(
        step_kernel,
        out_shape=(
            jax.ShapeDtypeStruct((1, mine, feat), bf16),
            jax.ShapeDtypeStruct((1, mine, feat), bf16),
            jax.ShapeDtypeStruct((1, BLK, hid), bf16),
        ),
        in_specs=[pl.BlockSpec(memory_space=pltpu.SMEM), vmem, vmem, vmem, vmem] + [anyw] * 4,
        out_specs=(vmem, vmem, vmem),
        scratch_shapes=[
            pltpu.VMEM((2, 2, rows, feat), bf16),
            pltpu.VMEM((slots, mine, feat), bf16),
            pltpu.VMEM((slots, BLK, hid), bf16),
            pltpu.VMEM((2, 2, 8, mine), f32),
            pltpu.VMEM((2, 2, 3, 8, mine), f32),
            pltpu.VMEM((2, mine, mine), f32),
            pltpu.VMEM((2, 2, mine, feat), bf16),
            pltpu.VMEM((2, 2, mine, feat), bf16),
            pltpu.VMEM((PIECES, mine // PIECES, feat), bf16),
            pltpu.VMEM((mine, feat), f32),
            pltpu.VMEM((mine, feat), bf16),
            pltpu.VMEM((mine, feat), bf16),
            pltpu.VMEM((3, mine, feat), bf16),
            pltpu.VMEM((3, mine, feat), bf16),
            pltpu.VMEM((tiles, feat, ft), bf16),
            pltpu.VMEM((tiles, ft, feat), bf16),
            pltpu.VMEM((2, LOCAL, rows, ft), bf16),
            pltpu.VMEM((2, SLOTS, 2, 2 * BLK, ft), bf16),
            pltpu.VMEM((2, SLOTS, 2, 4 * BLK, ft), bf16),
            pltpu.VMEM((2, LOCAL, 4 * BLK, ft), bf16),
            pltpu.VMEM((2, SLOTS, 2, BLK // 2, ft), bf16),
            pltpu.VMEM((2, SLOTS, 2, BLK, ft), bf16),
            pltpu.VMEM((2, SLOTS, SIDE, SIDE, BLK, ft), bf16),
            pltpu.VMEM((2, 2, rows, feat), f32),
            pltpu.SemaphoreType.DMA((4, 2, LOCAL)),
            pltpu.SemaphoreType.DMA((8, 2, SLOTS)),
            pltpu.SemaphoreType.DMA((tiles,)),
            pltpu.SemaphoreType.DMA((tiles,)),
            pltpu.SemaphoreType.DMA((2,)),
            pltpu.SemaphoreType.DMA((FRONT + 3 * PIECES + 3 * PARTS,)),
            pltpu.SemaphoreType.DMA((FRONT + 3 * PIECES + 3 * PARTS,)),
        ],
        compiler_params=pltpu.CompilerParams(
            collective_id=0, has_side_effects=True, vmem_limit_bytes=67043328
        ),
        name="section_step",
    )(plan, grad_in, ln_gain, b_in, b_out, stash_inputs, stash_hidden, w_in, w_out)
    return pl.pallas_call(
        store_kernel,
        out_shape=tuple(jax.ShapeDtypeStruct(r.shape, r.dtype) for r in results),
        in_specs=[anyw] * 3,
        out_specs=(anyw,) * 3,
        scratch_shapes=[pltpu.VMEM(r.shape, r.dtype) for r in results]
        + [pltpu.SemaphoreType.DMA((3,))] * 2,
        compiler_params=pltpu.CompilerParams(vmem_limit_bytes=67043328),
        name="store",
    )(*results)


def solution(mesh):
    in_specs = (
        P("section", None, "row", "col"),
        P("section", None, "col", "row"),
        P("section", "row", "col"),
        P("section", "col", "row"),
        P("section", "row"),
        P("section", "row", "col"),
        P("section", "col"),
        P("section", "col"),
        P("section", None),
    )
    out_specs = (P("section", "row", "col"), P("section", "row", "col"), P("section", "col", "row"))
    return jax.shard_map(body, mesh=mesh, in_specs=in_specs, out_specs=out_specs, check_vma=False)
```

```python
import jax
import jax.numpy as jnp
from jax import lax
from jax.experimental import pallas as pl
from jax.experimental.pallas import tpu as pltpu
from jax.sharding import PartitionSpec as P

D = 12288
FT = 512
SIDE = 4
SLOTS = 8
LOCAL = 4
BLK = 32
LATE_STAGE = 8
PIECES = 4
PARTS = 3
FRONT = 32

epsilon = 1e-05
root_coef = 0.7978845608028654
cubic_coef = 0.044715

RB1, LR1, RB2, LR2, A1, AR1, A2, AR2 = range(8)
SEND_RING = (0, 0, 1, 1, 2, 2, 3, 3)


def gelu_value(values):
    inner = root_coef * (values + cubic_coef * values * values * values)
    return 0.5 * values * (1.0 + jnp.tanh(inner))


def gelu_slope(values):
    inner = root_coef * (values + cubic_coef * values * values * values)
    tangent = jnp.tanh(inner)
    return 0.5 * (1.0 + tangent) + 0.5 * values * (1.0 - tangent * tangent) * root_coef * (
        1.0 + 3.0 * cubic_coef * values * values
    )


def dot_nn(a, b):
    return jnp.dot(a, b, preferred_element_type=jnp.float32)


def dot_nt(a, b):
    return lax.dot_general(a, b, (((1,), (1,)), ((), ())), preferred_element_type=jnp.float32)


class Copy:
    def __init__(self, *args):
        self.args = args

    def make(self):
        src, dst, send, recv, dev = self.args
        return pltpu.make_async_remote_copy(
            src_ref=src,
            dst_ref=dst,
            send_sem=send,
            recv_sem=recv,
            device_id=dev,
            device_id_type=pl.DeviceIdType.MESH,
        )

    def start(self):
        self.make().start()

    def wait_recv(self):
        self.make().wait_recv()

    def wait_recv_into(self, dst):
        src, _, send, recv, dev = self.args
        Copy(dst, dst, send, recv, dev).wait_recv()

    def wait_send(self):
        self.make().wait_send()


def step_kernel(
    plan,
    grad_h,
    gain_h,
    b_in_h,
    b_out_h,
    stash_x,
    stash_h,
    w_in,
    w_out,
    act_recv,
    grad_recv,
    saved,
    grad,
    gain,
    b_in,
    b_out,
    lhs,
    xs,
    stash,
    stat_src,
    stat_in,
    stats,
    pair_src,
    pair_in,
    relay_in,
    own_sum,
    far_src,
    far_in,
    sect_src,
    sect_in,
    win_s,
    wout_s,
    parts,
    rb1,
    lr1,
    quart,
    rb2,
    lr2,
    gath,
    acc,
    send_sem,
    recv_sem,
    win_sem,
    wout_sem,
    load_sem,
    side_send,
    side_recv,
):
    n_pair = win_s.shape[0] // 2
    ft = win_s.shape[2]
    units = 2 * n_pair
    f32, bf16 = jnp.float32, jnp.bfloat16
    col = lax.axis_index("col")
    pos = (col // SIDE, lax.rem(col, SIDE))

    def wrap(v):
        return jnp.bitwise_and(v + SIDE, SIDE - 1)

    along = (
        [{"col": wrap(pos[0] + by) * SIDE + pos[1]} for by in (1, 2, 3)],
        [{"col": pos[0] * SIDE + wrap(pos[1] + by)} for by in (1, 2, 3)],
    )
    hops = tuple((ring[0], ring[2]) for ring in along)
    places = tuple((p, wrap(p + 1), wrap(p + 2), wrap(p + 3)) for p in pos)

    def slot(u):
        return jnp.bitwise_and(u, SLOTS - 1)

    def local(u):
        return jnp.bitwise_and(u, LOCAL - 1)

    def win_copy(t):
        return pltpu.make_async_copy(
            w_in.at[0, :, pl.ds(pl.multiple_of(t * ft, ft), ft)], win_s.at[t], win_sem.at[t]
        )

    def wout_copy(t):
        return pltpu.make_async_copy(
            w_out.at[0, pl.ds(pl.multiple_of(t * ft, ft), ft), :], wout_s.at[t], wout_sem.at[t]
        )

    rows = SIDE * BLK
    feat = win_s.shape[1]
    row = lax.axis_index("row")
    high, core = row // 2, lax.rem(row, 2)
    section = lax.axis_index("section")
    mate = {"row": high * 2 + 1 - core}
    far = {"row": (1 - high) * 2 + core}
    next_same = {"section": 1 - section, "row": row}
    next_far = {"section": 1 - section, "row": (1 - high) * 2 + core}
    everyone = [*along[0], *along[1], mate, far, next_same, next_far]

    def side(i, src, dst, dev):
        return Copy(src, dst, side_send.at[i], side_recv.at[i], dev)

    barrier = pltpu.get_barrier_semaphore()
    for dev in everyone:
        pl.semaphore_signal(barrier, inc=1, device_id=dev, device_id_type=pl.DeviceIdType.MESH)

    loads = [
        pltpu.make_async_copy(src, dst, load_sem.at[i])
        for i, (src, dst) in enumerate(
            (
                (grad_h, grad),
                (stash_x.at[0], xs),
                (gain_h, gain),
                (b_in_h, b_in),
                (b_out_h, b_out),
                (stash_h.at[0], stash),
            )
        )
    ]
    for c in loads[:-1]:
        c.start()

    @pl.loop(0, 2 * n_pair)
    def _(t):
        wout_copy(t).start()

    loads[-1].start()

    @pl.loop(0, 2 * n_pair)
    def _(t):
        win_copy(t).start()

    pl.semaphore_wait(barrier, len(everyone))
    loads[0].wait()

    def row_block(high_of, core_of):
        return pl.ds(pl.multiple_of((high_of * 2 + core_of) * rows, rows), rows)

    piece = rows // PIECES
    mine, far_rows = row_block(high, core), row_block(1 - high, core)
    grads = lhs.at[0, 0]

    def piece_of(block_high, n):
        return pl.ds(pl.multiple_of((block_high * 2 + core) * rows + n * piece, piece), piece)

    by_way = (next_same, next_far)
    to_mate = side(0, grad.at[0], grads.at[mine], mate)
    out_hops = [
        side(FRONT + n, grad.at[0, pl.ds(n * piece, piece)], relay_in.at[n], by_way[n % 2])
        for n in range(PIECES)
    ]
    on_hops = [
        side(
            FRONT + PIECES + n,
            relay_in.at[n],
            grads.at[piece_of((high, 1 - high)[n % 2], n)],
            by_way[1 - n % 2],
        )
        for n in range(PIECES)
    ]
    far_to_mate = [
        side(
            FRONT + 2 * PIECES + n,
            grads.at[piece_of(1 - high, n)],
            grads.at[piece_of(1 - high, n)],
            mate,
        )
        for n in range(PIECES)
    ]
    for c in out_hops + [to_mate]:
        c.start()
    lhs[0, 0, mine] = grad[0]
    for n in range(PIECES):
        out_hops[n].wait_recv()
        on_hops[n].start()

    def pack(columns):
        lane = lax.broadcasted_iota(jnp.int32, (rows, rows), 1)
        grid = jnp.zeros((rows, rows), f32)
        for i, c in enumerate(columns):
            grid = jnp.where(lane == i, c, grid)
        return grid.T[:8]

    def unpack(packed):
        return jnp.concatenate([packed] * (rows // 8), axis=0).T

    def stat_copies(n, axis):
        first = 8 + (2 * n + axis) * 3
        return [
            side(first + j - 1, stat_src.at[n, axis], stat_in.at[n, axis, j - 1], along[axis][j - 1])
            for j in (1, 2, 3)
        ]

    def stat_send(n, axis, value):
        stat_src[n, axis] = value
        for c in stat_copies(n, axis):
            c.start()

    def stat_total(n, axis):
        copies = stat_copies(n, axis)
        for c in copies:
            c.wait_recv()
        total = stat_src[n, axis]
        for j in (0, 1, 2):
            total = total + stat_in[n, axis, j]
        for c in copies:
            c.wait_send()
        return total

    def row_sum(v):
        return jnp.sum(v, axis=1, keepdims=True)

    def first_stats():
        for c in loads[1:-1]:
            c.wait()
        fwd_input = xs[plan[0, 1]].astype(f32)
        bwd_input = xs[plan[0, 0]].astype(f32)
        sums = [
            row_sum(fwd_input),
            row_sum(fwd_input * fwd_input),
            row_sum(bwd_input),
            row_sum(bwd_input * bwd_input),
        ]
        stat_send(0, 0, pack(sums))

    def swap_rows(k, r):
        for z in range(SIDE):
            lhs[k, 1, pl.ds(pl.multiple_of((z * SIDE + r) * BLK, BLK), BLK)] = lhs[
                k, 0, pl.ds(pl.multiple_of((r * SIDE + z) * BLK, BLK), BLK)
            ]

    far_row = (1 - high) * 2 + core
    mate_row, far_mate_row = high * 2 + 1 - core, (1 - high) * 2 + 1 - core
    swap_rows(0, row)
    to_mate.wait_recv()
    swap_rows(0, mate_row)
    for n in range(PIECES):
        on_hops[n].wait_recv_into(grads.at[piece_of(1 - high, n)])
        far_to_mate[n].start()
    swap_rows(0, far_row)
    for n in range(PIECES):
        far_to_mate[n].wait_recv()
    swap_rows(0, far_mate_row)

    def front_sent():
        for c in out_hops + on_hops + far_to_mate + [to_mate]:
            c.wait_send()

    def ring(q, phase):
        axis = (q + phase) % 2
        return places[axis], hops[axis]

    def copy(kind, q, u, d, src, dst, hop):
        return Copy(
            src,
            dst,
            send_sem.at[SEND_RING[kind], q, local(u)],
            recv_sem.at[kind, q, slot(u)],
            hop[d],
        )

    def arrived(kind, q, u, ref):
        Copy(ref, ref, send_sem.at[0, q, 0], recv_sem.at[kind, q, slot(u)], hops[0][0]).wait_recv()

    def all_sent(ring_no, q, u, ref):
        Copy(ref, ref, send_sem.at[ring_no, q, local(u)], recv_sem.at[0, q, 0], hops[0][0]).wait_send()

    def span(i, size, lo, n):
        return pl.ds(pl.multiple_of(i * size + lo, n), n)

    def scatter_first(buf, back, side_buf, size, kinds, place, hop, q, u):
        half = size // 2
        me, nxt, far_one, prv = place
        src, s = buf.at[q, local(u)], slot(u)
        copy(kinds[0], q, u, 0, src.at[span(far_one, size, 0, half)], back.at[q, s, 0], hop).start()
        copy(kinds[0], q, u, 1, src.at[span(far_one, size, half, half)], back.at[q, s, 1], hop).start()
        copy(kinds[1], q, u, 0, src.at[span(nxt, size, half, half)],
             side_buf.at[q, s, 0, pl.ds(half, half)], hop).start()
        copy(kinds[1], q, u, 1, src.at[span(prv, size, 0, half)],
             side_buf.at[q, s, 1, pl.ds(0, half)], hop).start()

    def scatter_relay(buf, back, side_buf, size, kinds, place, hop, q, u):
        half = size // 2
        me, nxt, far_one, prv = place
        l, s = local(u), slot(u)
        arrived(kinds[0], q, u, back.at[q, s])
        for d, (chunk, lo) in enumerate(((nxt, 0), (prv, half))):
            rows = span(chunk, size, lo, half)
            buf[q, l, rows] = (
                buf[q, l, rows].astype(f32) + back[q, s, d].astype(f32)
            ).astype(bf16)
            copy(kinds[1], q, u, d, buf.at[q, l, rows],
                 side_buf.at[q, s, d, pl.ds(lo, half)], hop).start()

    big, small = SIDE * BLK, BLK

    def s0(u, q):
        l = local(u)

        @pl.when(u < n_pair)
        def _():
            t = 2 * u + q
            wout_copy(t).wait()
            parts[q, l] = dot_nt(lhs[0, q], wout_s[t]).astype(bf16)

        @pl.when(u >= n_pair)
        def _():
            t = 2 * (u - n_pair) + q
            if n_pair < LATE_STAGE - 1:
                win_copy(t).wait()
            parts[q, l] = dot_nn(lhs[1, q], win_s[t]).astype(bf16)

        scatter_first(parts, rb1, lr1, big, (RB1, LR1), *ring(q, 0), q, u)

    def s1(u, q):
        scatter_relay(parts, rb1, lr1, big, (RB1, LR1), *ring(q, 0), q, u)

    def s2(u, q):
        place, _ = ring(q, 0)
        l, s = local(u), slot(u)
        arrived(LR1, q, u, lr1.at[q, s])
        quart[q, l] = (
            parts[q, l, span(place[0], big, 0, big)].astype(f32)
            + lr1[q, s, 0].astype(f32)
            + lr1[q, s, 1].astype(f32)
        ).astype(bf16)
        scatter_first(quart, rb2, lr2, small, (RB2, LR2), *ring(q, 1), q, u)
        all_sent(0, q, u, parts.at[q, l, pl.ds(0, 3 * big)])

    def s3(u, q):
        scatter_relay(quart, rb2, lr2, small, (RB2, LR2), *ring(q, 1), q, u)

    def s4(u, q):
        me1 = ring(q, 0)[0][0]
        place, hop = ring(q, 1)
        me2 = place[0]
        l, s = local(u), slot(u)
        arrived(LR2, q, u, lr2.at[q, s])
        h = (
            quart[q, l, span(me2, small, 0, small)].astype(f32)
            + lr2[q, s, 0].astype(f32)
            + lr2[q, s, 1].astype(f32)
        )

        @pl.when(u < n_pair)
        def _():
            t = 2 * u + q
            cols = pl.ds(pl.multiple_of(t * ft, ft), ft)
            slope = gelu_slope(stash[plan[0, 0], :, cols].astype(f32))
            gath[q, s, me1, me2] = (h * slope).astype(bf16)

        @pl.when(u >= n_pair)
        def _():
            t = 2 * (u - n_pair) + q
            cols = pl.ds(pl.multiple_of(t * ft, ft), ft)
            hidden = h + b_in[:, cols]
            saved[0, :, cols] = hidden.astype(bf16)
            gath[q, s, me1, me2] = gelu_value(hidden).astype(bf16)

        g = gath.at[q, s, me1, me2]
        for d in (0, 1):
            copy(A1, q, u, d, g, g, hop).start()
        all_sent(1, q, u, quart.at[q, l, pl.ds(0, 3 * small)])

    def s5(u, q):
        me1 = ring(q, 0)[0][0]
        place, hop = ring(q, 1)
        g = gath.at[q, slot(u), me1]
        arrived(A1, q, u, g.at[pl.ds(0, 2)])
        for d, (b, lo) in enumerate(((place[3], 0), (place[1], BLK // 2))):
            r = g.at[b, pl.ds(lo, BLK // 2)]
            copy(AR1, q, u, d, r, r, hop).start()

    def product(u, q, blocks):
        s = slot(u)

        def add(kind, first, values):
            @pl.when(first)
            def _():
                for b, value in zip(blocks, values):
                    acc[kind, q, span(b, big, 0, big)] = value

            @pl.when(jnp.logical_not(first))
            def _():
                for b, value in zip(blocks, values):
                    acc[kind, q, span(b, big, 0, big)] += value

        pieces = [gath[q, s, b].reshape(big, ft) for b in blocks]

        @pl.when(u < n_pair)
        def _():
            t = 2 * u + q
            add(0, u == 0, [dot_nt(piece, win_s[t]) for piece in pieces])

        @pl.when(u >= n_pair)
        def _():
            t = 2 * (u - n_pair) + q
            add(1, u == n_pair, [dot_nn(piece, wout_s[t]) for piece in pieces])

    def s6(u, q):
        place, hop = ring(q, 0)
        me1 = place[0]
        g = gath.at[q, slot(u)]
        arrived(AR1, q, u, g.at[me1, 0])
        for d in (0, 1):
            copy(A2, q, u, d, g.at[me1], g.at[me1], hop).start()
        if n_pair >= LATE_STAGE - 1:

            @pl.when(u < n_pair)
            def _():
                win_copy(2 * u + q).wait()

        product(u, q, [me1])
        all_sent(2, q, u, g.at[me1, pl.ds(0, 3)])

    def s7(u, q):
        place, hop = ring(q, 0)
        g = gath.at[q, slot(u)]
        arrived(A2, q, u, g.at[pl.ds(0, 2)])
        for d, (b, lo) in enumerate(((place[3], 0), (place[1], SIDE // 2))):
            r = g.at[b, pl.ds(lo, SIDE // 2)]
            copy(AR2, q, u, d, r, r, hop).start()
        product(u, q, [place[1], place[3]])

    def s8(u, q):
        place, _ = ring(q, 0)
        g = gath.at[q, slot(u)]
        arrived(AR2, q, u, g.at[0])
        product(u, q, [place[2]])
        all_sent(3, q, u, g.at[pl.ds(0, 3)])

    stages = (s0, s1, s2, s3, s4, s5, s6, s7, s8)
    normed_rows = lhs.at[1, 0]
    base = 20
    normed_to_mate = side(base, normed_rows.at[mine], normed_rows.at[mine], mate)
    normed_to_far = side(base + 1, normed_rows.at[mine], normed_rows.at[mine], far)
    normed_on = side(base + 2, normed_rows.at[far_rows], normed_rows.at[far_rows], mate)
    pair_sum = side(base + 3, pair_src.at[0], pair_in.at[0], mate)
    far_sum = side(base + 5, far_src, far_in, far)
    grad_on = side(base + 6, sect_src.at[0], sect_in.at[0], next_same)
    wide = feat // PARTS
    cuts = [pl.ds(p * wide, wide) for p in range(PARTS)]
    tail = FRONT + 3 * PIECES
    pair_parts = [
        side(tail + p, pair_src.at[1, :, :, c], pair_in.at[1, :, :, c], mate)
        for p, c in enumerate(cuts)
    ]
    act_parts = [
        [
            side(
                tail + PARTS + 2 * p + n,
                sect_src.at[1 + n, :, c],
                sect_in.at[1 + n, :, c],
                by_way[n],
            )
            for n in (0, 1)
        ]
        for p, c in enumerate(cuts)
    ]

    def total_rows(k, high_of, core_of, cut):
        r = high_of * 2 + core_of
        pieces = []
        for z in range(SIDE):
            own = pl.ds(pl.multiple_of((r * SIDE + z) * BLK, BLK), BLK)
            swap = pl.ds(pl.multiple_of((z * SIDE + r) * BLK, BLK), BLK)
            pieces.append(acc[k, 0, own, cut] + acc[k, 1, swap, cut])
        return jnp.concatenate(pieces, axis=0)

    def pair_part(k, cut):
        for h in (0, 1):
            pair_src[k, h, :, cut] = total_rows(k, h, 1 - core, cut).astype(bf16)

    def chip_rows(k, high_of, cut):
        return total_rows(k, high_of, core, cut) + pair_in[k, high_of, :, cut].astype(f32)

    def grad_pair():
        pair_part(0, slice(None))
        pair_sum.start()

    def norm_stats():
        stat_send(0, 1, stat_total(0, 0))

    def normalize():
        total = unpack(stat_total(0, 1)) / D
        mean_f, mean_b = total[:, 0:1], total[:, 2:3]
        inv_f = lax.rsqrt(total[:, 1:2] - mean_f * mean_f + epsilon)
        inv_b = lax.rsqrt(total[:, 3:4] - mean_b * mean_b + epsilon)
        stats[0] = jnp.broadcast_to(mean_b, (rows, rows))
        stats[1] = jnp.broadcast_to(inv_b, (rows, rows))
        values = xs[plan[0, 1]].astype(f32)
        lhs[1, 0, mine] = ((values - mean_f) * inv_f * gain[...]).astype(bf16)
        normed_to_mate.start()
        normed_to_far.start()

    def normed_forward():
        normed_to_far.wait_recv_into(normed_rows.at[far_rows])
        normed_on.start()

    def normed_done():
        normed_to_mate.wait_recv()
        normed_on.wait_recv()
        for r in (row, mate_row, far_row, far_mate_row):
            swap_rows(1, r)
        for c in (normed_to_mate, normed_to_far, normed_on):
            c.wait_send()

    def grad_far():
        pair_sum.wait_recv()
        own_sum[...] = chip_rows(0, high, slice(None))
        far_src[...] = chip_rows(0, 1 - high, slice(None)).astype(bf16)
        far_sum.start()
        pair_sum.wait_send()

    def hat():
        return (xs[plan[0, 0]].astype(f32) - stats[0, :, 0:1]) * stats[1, :, 0:1]

    def grad_stats():
        far_sum.wait_recv()
        scaled = (own_sum[...] + far_in[...].astype(f32)) * gain[...]
        own_sum[...] = scaled
        stat_send(1, 0, pack([row_sum(scaled), row_sum(scaled * hat())]))
        far_sum.wait_send()

    def grad_stats_more():
        stat_send(1, 1, stat_total(1, 0))

    def grad_out():
        total = unpack(stat_total(1, 1)) / D
        in_grad = grad[0].astype(f32) + stats[1, :, 0:1] * (
            own_sum[...] - total[:, 0:1] - hat() * total[:, 1:2]
        )
        sect_src[0] = in_grad.astype(bf16)
        grad_on.start()

    last = n_pair + len(stages) - 2
    early = (2, 4, 7, 9) if n_pair >= 10 else (1, 2, 4, 5)
    jobs = (
        (0, 0, first_stats),
        (1, 0, front_sent),
        (3, 3, loads[-1].wait),
        (early[0], 0, norm_stats),
        (early[1], 0, normalize),
        (early[2], 0, normed_forward),
        (early[3], 0, normed_done),
        (last, 8, grad_pair),
        (last + 1, 3, grad_far),
        (last + 3, 3, grad_stats),
        (last + 4, 0, grad_stats_more),
        (last + 4, 7, grad_out),
    )

    @pl.loop(0, units + len(stages) - 1)
    def _(step):
        for k, stage in enumerate(stages):
            u = step - k

            @pl.when(jnp.logical_and(u >= 0, u < units))
            def _():
                for q in (0, 1):
                    stage(u, q)

            for at, after, job in jobs:
                if after == k:
                    pl.when(step == at)(job)

    for p, c in enumerate(cuts):
        pair_part(1, c)
        pair_parts[p].start()
    for p, c in enumerate(cuts):
        pair_parts[p].wait_recv()
        sect_src[2, :, c] = chip_rows(1, 1 - high, c).astype(bf16)
        act_parts[p][1].start()
        residual = xs[plan[0, 1], :, c].astype(f32) + b_out[:, c]
        sect_src[1, :, c] = (chip_rows(1, high, c) + residual).astype(bf16)
        act_parts[p][0].start()
    grad_on.wait_recv()
    grad_recv[0] = sect_in[0]
    for p, c in enumerate(cuts):
        for n in (0, 1):
            act_parts[p][n].wait_recv()
        act_recv[0, :, c] = (
            sect_in[1, :, c].astype(f32) + sect_in[2, :, c].astype(f32)
        ).astype(bf16)
    for c in pair_parts + act_parts[0] + act_parts[1] + act_parts[2] + [grad_on]:
        c.wait_send()


def store_kernel(*refs):
    n = len(refs) // 2
    copies = [
        pltpu.make_async_copy(refs[i], refs[n + i], refs[-1].at[i]) for i in range(n)
    ]
    for c in copies:
        c.start()
    for c in copies:
        c.wait()


def body(stash_inputs, stash_hidden, grad_in, w_in, b_in, w_out, b_out, ln_gain, plan, ft=FT):
    _, feat, hid = w_in.shape
    slots = stash_inputs.shape[1]
    tiles = hid // ft
    rows, mine = SIDE * SIDE * BLK, SIDE * BLK
    bf16, f32 = jnp.bfloat16, jnp.float32
    vmem, anyw = pl.BlockSpec(memory_space=pltpu.VMEM), pl.BlockSpec(memory_space=pl.ANY)
    results = pl.pallas_call(
        step_kernel,
        out_shape=(
            pltpu.VMEM((1, mine, feat), bf16),
            pltpu.VMEM((1, mine, feat), bf16),
            pltpu.VMEM((1, BLK, hid), bf16),
        ),
        in_specs=[pl.BlockSpec(memory_space=pltpu.SMEM)] + [anyw] * 8,
        out_specs=(vmem, vmem, vmem),
        scratch_shapes=[
            *(pltpu.VMEM(v.shape, v.dtype) for v in (grad_in, ln_gain, b_in, b_out)),
            pltpu.VMEM((2, 2, rows, feat), bf16),
            pltpu.VMEM((slots, mine, feat), bf16),
            pltpu.VMEM((slots, BLK, hid), bf16),
            pltpu.VMEM((2, 2, 8, mine), f32),
            pltpu.VMEM((2, 2, 3, 8, mine), f32),
            pltpu.VMEM((2, mine, mine), f32),
            pltpu.VMEM((2, 2, mine, feat), bf16),
            pltpu.VMEM((2, 2, mine, feat), bf16),
            pltpu.VMEM((PIECES, mine // PIECES, feat), bf16),
            pltpu.VMEM((mine, feat), f32),
            pltpu.VMEM((mine, feat), bf16),
            pltpu.VMEM((mine, feat), bf16),
            pltpu.VMEM((3, mine, feat), bf16),
            pltpu.VMEM((3, mine, feat), bf16),
            pltpu.VMEM((tiles, feat, ft), bf16),
            pltpu.VMEM((tiles, ft, feat), bf16),
            pltpu.VMEM((2, LOCAL, rows, ft), bf16),
            pltpu.VMEM((2, SLOTS, 2, 2 * BLK, ft), bf16),
            pltpu.VMEM((2, SLOTS, 2, 4 * BLK, ft), bf16),
            pltpu.VMEM((2, LOCAL, 4 * BLK, ft), bf16),
            pltpu.VMEM((2, SLOTS, 2, BLK // 2, ft), bf16),
            pltpu.VMEM((2, SLOTS, 2, BLK, ft), bf16),
            pltpu.VMEM((2, SLOTS, SIDE, SIDE, BLK, ft), bf16),
            pltpu.VMEM((2, 2, rows, feat), f32),
            pltpu.SemaphoreType.DMA((4, 2, LOCAL)),
            pltpu.SemaphoreType.DMA((8, 2, SLOTS)),
            pltpu.SemaphoreType.DMA((tiles,)),
            pltpu.SemaphoreType.DMA((tiles,)),
            pltpu.SemaphoreType.DMA((6,)),
            pltpu.SemaphoreType.DMA((FRONT + 3 * PIECES + 3 * PARTS,)),
            pltpu.SemaphoreType.DMA((FRONT + 3 * PIECES + 3 * PARTS,)),
        ],
        compiler_params=pltpu.CompilerParams(
            collective_id=0, has_side_effects=True, vmem_limit_bytes=60 << 20
        ),
        name="section_step",
    )(plan, grad_in, ln_gain, b_in, b_out, stash_inputs, stash_hidden, w_in, w_out)
    return pl.pallas_call(
        store_kernel,
        out_shape=tuple(jax.ShapeDtypeStruct(r.shape, r.dtype) for r in results),
        in_specs=[vmem] * 3,
        out_specs=(anyw,) * 3,
        scratch_shapes=[pltpu.SemaphoreType.DMA((3,))],
        compiler_params=pltpu.CompilerParams(vmem_limit_bytes=4 << 20),
        name="store",
    )(*results)


def solution(mesh):
    in_specs = (
        P("section", None, "row", "col"),
        P("section", None, "col", "row"),
        P("section", "row", "col"),
        P("section", "col", "row"),
        P("section", "row"),
        P("section", "row", "col"),
        P("section", "col"),
        P("section", "col"),
        P("section", None),
    )
    out_specs = (P("section", "row", "col"), P("section", "row", "col"), P("section", "col", "row"))
    return jax.shard_map(body, mesh=mesh, in_specs=in_specs, out_specs=out_specs, check_vma=False)
```

```python
import jax
import jax.numpy as jnp
from jax import lax
from jax.experimental import pallas as pl
from jax.experimental.pallas import tpu as pltpu
from jax.sharding import PartitionSpec as P

D = 12288
FT = 512
SIDE = 4
SLOTS = 8
LOCAL = 4
BLK = 32
LATE_STAGE = 8
PIECES = 4
FRONT = 32

epsilon = 1e-05
root_coef = 0.7978845608028654
cubic_coef = 0.044715

RB1, LR1, RB2, LR2, A1, AR1, A2, AR2 = range(8)
SEND_RING = (0, 0, 1, 1, 2, 2, 3, 3)


def gelu_value(values):
    inner = root_coef * (values + cubic_coef * values * values * values)
    return 0.5 * values * (1.0 + jnp.tanh(inner))


def gelu_slope(values):
    inner = root_coef * (values + cubic_coef * values * values * values)
    tangent = jnp.tanh(inner)
    return 0.5 * (1.0 + tangent) + 0.5 * values * (1.0 - tangent * tangent) * root_coef * (
        1.0 + 3.0 * cubic_coef * values * values
    )


def dot_nn(a, b):
    return jnp.dot(a, b, preferred_element_type=jnp.float32)


def dot_nt(a, b):
    return lax.dot_general(a, b, (((1,), (1,)), ((), ())), preferred_element_type=jnp.float32)


class Copy:
    def __init__(self, *args):
        self.args = args

    def make(self):
        src, dst, send, recv, dev = self.args
        return pltpu.make_async_remote_copy(
            src_ref=src,
            dst_ref=dst,
            send_sem=send,
            recv_sem=recv,
            device_id=dev,
            device_id_type=pl.DeviceIdType.MESH,
        )

    def start(self):
        self.make().start()

    def wait_recv(self):
        self.make().wait_recv()

    def wait_recv_into(self, dst):
        src, _, send, recv, dev = self.args
        Copy(dst, dst, send, recv, dev).wait_recv()

    def wait_send(self):
        self.make().wait_send()


def step_kernel(
    plan,
    grad_h,
    gain_h,
    b_in_h,
    b_out_h,
    stash_x,
    stash_h,
    w_in,
    w_out,
    act_recv,
    grad_recv,
    saved,
    grad,
    gain,
    b_in,
    b_out,
    lhs,
    xs,
    stash,
    stat_src,
    stat_in,
    stats,
    pair_src,
    pair_in,
    relay_in,
    own_sum,
    far_src,
    far_in,
    sect_src,
    sect_in,
    win_s,
    wout_s,
    parts,
    rb1,
    lr1,
    quart,
    rb2,
    lr2,
    gath,
    acc,
    send_sem,
    recv_sem,
    win_sem,
    wout_sem,
    load_sem,
    side_send,
    side_recv,
):
    n_pair = win_s.shape[0] // 2
    ft = win_s.shape[2]
    units = 2 * n_pair
    f32, bf16 = jnp.float32, jnp.bfloat16
    col = lax.axis_index("col")
    pos = (col // SIDE, lax.rem(col, SIDE))

    def wrap(v):
        return jnp.bitwise_and(v + SIDE, SIDE - 1)

    along = (
        [{"col": wrap(pos[0] + by) * SIDE + pos[1]} for by in (1, 2, 3)],
        [{"col": pos[0] * SIDE + wrap(pos[1] + by)} for by in (1, 2, 3)],
    )
    hops = tuple((ring[0], ring[2]) for ring in along)
    places = tuple((p, wrap(p + 1), wrap(p + 2), wrap(p + 3)) for p in pos)

    def slot(u):
        return jnp.bitwise_and(u, SLOTS - 1)

    def local(u):
        return jnp.bitwise_and(u, LOCAL - 1)

    def win_copy(t):
        return pltpu.make_async_copy(
            w_in.at[0, :, pl.ds(pl.multiple_of(t * ft, ft), ft)], win_s.at[t], win_sem.at[t]
        )

    def wout_copy(t):
        return pltpu.make_async_copy(
            w_out.at[0, pl.ds(pl.multiple_of(t * ft, ft), ft), :], wout_s.at[t], wout_sem.at[t]
        )

    rows = SIDE * BLK
    feat = win_s.shape[1]
    row = lax.axis_index("row")
    high, core = row // 2, lax.rem(row, 2)
    section = lax.axis_index("section")
    mate = {"row": high * 2 + 1 - core}
    far = {"row": (1 - high) * 2 + core}
    next_same = {"section": 1 - section, "row": row}
    next_far = {"section": 1 - section, "row": (1 - high) * 2 + core}
    everyone = [*along[0], *along[1], mate, far, next_same, next_far]

    def side(i, src, dst, dev):
        return Copy(src, dst, side_send.at[i], side_recv.at[i], dev)

    barrier = pltpu.get_barrier_semaphore()
    for dev in everyone:
        pl.semaphore_signal(barrier, inc=1, device_id=dev, device_id_type=pl.DeviceIdType.MESH)

    loads = [
        pltpu.make_async_copy(src, dst, load_sem.at[i])
        for i, (src, dst) in enumerate(
            (
                (grad_h, grad),
                (stash_x.at[0], xs),
                (gain_h, gain),
                (b_in_h, b_in),
                (b_out_h, b_out),
                (stash_h.at[0], stash),
            )
        )
    ]
    for c in loads[:-1]:
        c.start()

    @pl.loop(0, 2 * n_pair)
    def _(t):
        wout_copy(t).start()

    loads[-1].start()

    @pl.loop(0, 2 * n_pair)
    def _(t):
        win_copy(t).start()

    pl.semaphore_wait(barrier, len(everyone))
    loads[0].wait()

    def row_block(high_of, core_of):
        return pl.ds(pl.multiple_of((high_of * 2 + core_of) * rows, rows), rows)

    piece = rows // PIECES
    mine, far_rows = row_block(high, core), row_block(1 - high, core)
    grads = lhs.at[0, 0]

    def piece_of(block_high, n):
        return pl.ds(pl.multiple_of((block_high * 2 + core) * rows + n * piece, piece), piece)

    by_way = (next_same, next_far)
    to_mate = side(0, grad.at[0], grads.at[mine], mate)
    out_hops = [
        side(FRONT + n, grad.at[0, pl.ds(n * piece, piece)], relay_in.at[n], by_way[n % 2])
        for n in range(PIECES)
    ]
    on_hops = [
        side(
            FRONT + PIECES + n,
            relay_in.at[n],
            grads.at[piece_of((high, 1 - high)[n % 2], n)],
            by_way[1 - n % 2],
        )
        for n in range(PIECES)
    ]
    far_to_mate = [
        side(
            FRONT + 2 * PIECES + n,
            grads.at[piece_of(1 - high, n)],
            grads.at[piece_of(1 - high, n)],
            mate,
        )
        for n in range(PIECES)
    ]
    for c in out_hops + [to_mate]:
        c.start()
    lhs[0, 0, mine] = grad[0]
    for n in range(PIECES):
        out_hops[n].wait_recv()
        on_hops[n].start()

    def pack(columns):
        lane = lax.broadcasted_iota(jnp.int32, (rows, rows), 1)
        grid = jnp.zeros((rows, rows), f32)
        for i, c in enumerate(columns):
            grid = jnp.where(lane == i, c, grid)
        return grid.T[:8]

    def unpack(packed):
        return jnp.concatenate([packed] * (rows // 8), axis=0).T

    def stat_copies(n, axis):
        first = 8 + (2 * n + axis) * 3
        return [
            side(first + j - 1, stat_src.at[n, axis], stat_in.at[n, axis, j - 1], along[axis][j - 1])
            for j in (1, 2, 3)
        ]

    def stat_send(n, axis, value):
        stat_src[n, axis] = value
        for c in stat_copies(n, axis):
            c.start()

    def stat_total(n, axis):
        copies = stat_copies(n, axis)
        for c in copies:
            c.wait_recv()
        total = stat_src[n, axis]
        for j in (0, 1, 2):
            total = total + stat_in[n, axis, j]
        for c in copies:
            c.wait_send()
        return total

    def row_sum(v):
        return jnp.sum(v, axis=1, keepdims=True)

    def first_stats():
        for c in loads[1:-1]:
            c.wait()
        fwd_input = xs[plan[0, 1]].astype(f32)
        bwd_input = xs[plan[0, 0]].astype(f32)
        sums = [
            row_sum(fwd_input),
            row_sum(fwd_input * fwd_input),
            row_sum(bwd_input),
            row_sum(bwd_input * bwd_input),
        ]
        stat_send(0, 0, pack(sums))

    def swap_rows(k, r):
        for z in range(SIDE):
            lhs[k, 1, pl.ds(pl.multiple_of((z * SIDE + r) * BLK, BLK), BLK)] = lhs[
                k, 0, pl.ds(pl.multiple_of((r * SIDE + z) * BLK, BLK), BLK)
            ]

    far_row = (1 - high) * 2 + core
    mate_row, far_mate_row = high * 2 + 1 - core, (1 - high) * 2 + 1 - core
    swap_rows(0, row)
    to_mate.wait_recv()
    swap_rows(0, mate_row)
    for n in range(PIECES):
        on_hops[n].wait_recv_into(grads.at[piece_of(1 - high, n)])
        far_to_mate[n].start()
    swap_rows(0, far_row)
    for n in range(PIECES):
        far_to_mate[n].wait_recv()
    swap_rows(0, far_mate_row)

    def front_sent():
        for c in out_hops + on_hops + far_to_mate + [to_mate]:
            c.wait_send()

    def ring(q, phase):
        axis = (q + phase) % 2
        return places[axis], hops[axis]

    def copy(kind, q, u, d, src, dst, hop):
        return Copy(
            src,
            dst,
            send_sem.at[SEND_RING[kind], q, local(u)],
            recv_sem.at[kind, q, slot(u)],
            hop[d],
        )

    def arrived(kind, q, u, ref):
        Copy(ref, ref, send_sem.at[0, q, 0], recv_sem.at[kind, q, slot(u)], hops[0][0]).wait_recv()

    def all_sent(ring_no, q, u, ref):
        Copy(ref, ref, send_sem.at[ring_no, q, local(u)], recv_sem.at[0, q, 0], hops[0][0]).wait_send()

    def span(i, size, lo, n):
        return pl.ds(pl.multiple_of(i * size + lo, n), n)

    def scatter_first(buf, back, side_buf, size, kinds, place, hop, q, u):
        half = size // 2
        me, nxt, far_one, prv = place
        src, s = buf.at[q, local(u)], slot(u)
        copy(kinds[0], q, u, 0, src.at[span(far_one, size, 0, half)], back.at[q, s, 0], hop).start()
        copy(kinds[0], q, u, 1, src.at[span(far_one, size, half, half)], back.at[q, s, 1], hop).start()
        copy(kinds[1], q, u, 0, src.at[span(nxt, size, half, half)],
             side_buf.at[q, s, 0, pl.ds(half, half)], hop).start()
        copy(kinds[1], q, u, 1, src.at[span(prv, size, 0, half)],
             side_buf.at[q, s, 1, pl.ds(0, half)], hop).start()

    def scatter_relay(buf, back, side_buf, size, kinds, place, hop, q, u):
        half = size // 2
        me, nxt, far_one, prv = place
        l, s = local(u), slot(u)
        arrived(kinds[0], q, u, back.at[q, s])
        for d, (chunk, lo) in enumerate(((nxt, 0), (prv, half))):
            rows = span(chunk, size, lo, half)
            buf[q, l, rows] = (
                buf[q, l, rows].astype(f32) + back[q, s, d].astype(f32)
            ).astype(bf16)
            copy(kinds[1], q, u, d, buf.at[q, l, rows],
                 side_buf.at[q, s, d, pl.ds(lo, half)], hop).start()

    big, small = SIDE * BLK, BLK

    def s0(u, q):
        l = local(u)

        @pl.when(u < n_pair)
        def _():
            t = 2 * u + q
            wout_copy(t).wait()
            parts[q, l] = dot_nt(lhs[0, q], wout_s[t]).astype(bf16)

        @pl.when(u >= n_pair)
        def _():
            t = 2 * (u - n_pair) + q
            if n_pair < LATE_STAGE - 1:
                win_copy(t).wait()
            parts[q, l] = dot_nn(lhs[1, q], win_s[t]).astype(bf16)

        scatter_first(parts, rb1, lr1, big, (RB1, LR1), *ring(q, 0), q, u)

    def s1(u, q):
        scatter_relay(parts, rb1, lr1, big, (RB1, LR1), *ring(q, 0), q, u)

    def s2(u, q):
        place, _ = ring(q, 0)
        l, s = local(u), slot(u)
        arrived(LR1, q, u, lr1.at[q, s])
        quart[q, l] = (
            parts[q, l, span(place[0], big, 0, big)].astype(f32)
            + lr1[q, s, 0].astype(f32)
            + lr1[q, s, 1].astype(f32)
        ).astype(bf16)
        scatter_first(quart, rb2, lr2, small, (RB2, LR2), *ring(q, 1), q, u)
        all_sent(0, q, u, parts.at[q, l, pl.ds(0, 3 * big)])

    def s3(u, q):
        scatter_relay(quart, rb2, lr2, small, (RB2, LR2), *ring(q, 1), q, u)

    def s4(u, q):
        me1 = ring(q, 0)[0][0]
        place, hop = ring(q, 1)
        me2 = place[0]
        l, s = local(u), slot(u)
        arrived(LR2, q, u, lr2.at[q, s])
        h = (
            quart[q, l, span(me2, small, 0, small)].astype(f32)
            + lr2[q, s, 0].astype(f32)
            + lr2[q, s, 1].astype(f32)
        )

        @pl.when(u < n_pair)
        def _():
            t = 2 * u + q
            cols = pl.ds(pl.multiple_of(t * ft, ft), ft)
            slope = gelu_slope(stash[plan[0, 0], :, cols].astype(f32))
            gath[q, s, me1, me2] = (h * slope).astype(bf16)

        @pl.when(u >= n_pair)
        def _():
            t = 2 * (u - n_pair) + q
            cols = pl.ds(pl.multiple_of(t * ft, ft), ft)
            hidden = h + b_in[:, cols]
            saved[0, :, cols] = hidden.astype(bf16)
            gath[q, s, me1, me2] = gelu_value(hidden).astype(bf16)

        g = gath.at[q, s, me1, me2]
        for d in (0, 1):
            copy(A1, q, u, d, g, g, hop).start()
        all_sent(1, q, u, quart.at[q, l, pl.ds(0, 3 * small)])

    def s5(u, q):
        me1 = ring(q, 0)[0][0]
        place, hop = ring(q, 1)
        g = gath.at[q, slot(u), me1]
        arrived(A1, q, u, g.at[pl.ds(0, 2)])
        for d, (b, lo) in enumerate(((place[3], 0), (place[1], BLK // 2))):
            r = g.at[b, pl.ds(lo, BLK // 2)]
            copy(AR1, q, u, d, r, r, hop).start()

    def product(u, q, blocks):
        s = slot(u)

        def add(kind, first, values):
            @pl.when(first)
            def _():
                for b, value in zip(blocks, values):
                    acc[kind, q, span(b, big, 0, big)] = value

            @pl.when(jnp.logical_not(first))
            def _():
                for b, value in zip(blocks, values):
                    acc[kind, q, span(b, big, 0, big)] += value

        pieces = [gath[q, s, b].reshape(big, ft) for b in blocks]

        @pl.when(u < n_pair)
        def _():
            t = 2 * u + q
            add(0, u == 0, [dot_nt(piece, win_s[t]) for piece in pieces])

        @pl.when(u >= n_pair)
        def _():
            t = 2 * (u - n_pair) + q
            add(1, u == n_pair, [dot_nn(piece, wout_s[t]) for piece in pieces])

    def s6(u, q):
        place, hop = ring(q, 0)
        me1 = place[0]
        g = gath.at[q, slot(u)]
        arrived(AR1, q, u, g.at[me1, 0])
        for d in (0, 1):
            copy(A2, q, u, d, g.at[me1], g.at[me1], hop).start()
        if n_pair >= LATE_STAGE - 1:

            @pl.when(u < n_pair)
            def _():
                win_copy(2 * u + q).wait()

        product(u, q, [me1])
        all_sent(2, q, u, g.at[me1, pl.ds(0, 3)])

    def s7(u, q):
        place, hop = ring(q, 0)
        g = gath.at[q, slot(u)]
        arrived(A2, q, u, g.at[pl.ds(0, 2)])
        for d, (b, lo) in enumerate(((place[3], 0), (place[1], SIDE // 2))):
            r = g.at[b, pl.ds(lo, SIDE // 2)]
            copy(AR2, q, u, d, r, r, hop).start()
        product(u, q, [place[1], place[3]])

    def s8(u, q):
        place, _ = ring(q, 0)
        g = gath.at[q, slot(u)]
        arrived(AR2, q, u, g.at[0])
        product(u, q, [place[2]])
        all_sent(3, q, u, g.at[pl.ds(0, 3)])

    stages = (s0, s1, s2, s3, s4, s5, s6, s7, s8)
    normed_rows = lhs.at[1, 0]
    base = 20
    normed_to_mate = side(base, normed_rows.at[mine], normed_rows.at[mine], mate)
    normed_to_far = side(base + 1, normed_rows.at[mine], normed_rows.at[mine], far)
    normed_on = side(base + 2, normed_rows.at[far_rows], normed_rows.at[far_rows], mate)
    pair_sum = side(base + 3, pair_src.at[0], pair_in.at[0], mate)
    far_sum = side(base + 5, far_src, far_in, far)
    grad_on = side(base + 6, sect_src.at[0], sect_in.at[0], next_same)
    tail = FRONT + 3 * PIECES
    x_far = places[0][2]
    turns = tuple(places[1][i] for i in (0, 1, 3, 2))
    soon, late = pl.ds(0, 3 * BLK), pl.ds(3 * BLK, BLK)
    highs = (high, 1 - high)
    pair_parts = [
        [
            side(tail + 2 * n + i, pair_src.at[1, n, r], pair_in.at[1, n, r], mate)
            for i, r in enumerate((soon, late))
        ]
        for n in (0, 1)
    ]
    act_parts = [
        [
            side(tail + 4 + 2 * n + i, sect_src.at[1 + n, r], sect_in.at[1 + n, r], by_way[n])
            for i, r in enumerate((soon, late))
        ]
        for n in (0, 1)
    ]

    def token_rows(k, r, z):
        own = pl.ds(pl.multiple_of((r * SIDE + z) * BLK, BLK), BLK)
        swap = pl.ds(pl.multiple_of((z * SIDE + r) * BLK, BLK), BLK)
        return acc[k, 0, own] + acc[k, 1, swap]

    def total_rows(k, high_of, core_of):
        r = high_of * 2 + core_of
        return jnp.concatenate([token_rows(k, r, z) for z in range(SIDE)], axis=0)

    def chip_rows(k, high_of):
        return total_rows(k, high_of, core) + pair_in[k, high_of].astype(f32)

    def act_pair(n, i):
        for j in ((0, 1, 2), (3,))[i]:
            rows = token_rows(1, highs[n] * 2 + 1 - core, turns[j])
            pair_src[1, n, pl.ds(j * BLK, BLK)] = rows.astype(bf16)
        pair_parts[n][i].start()

    def act_out(n, i):
        pair_parts[n][i].wait_recv()
        for j in ((0, 1, 2), (3,))[i]:
            at = pl.ds(j * BLK, BLK)
            rows = token_rows(1, highs[n] * 2 + core, turns[j]) + pair_in[1, n, at].astype(f32)
            if n == 0:
                own = pl.ds(pl.multiple_of(turns[j] * BLK, BLK), BLK)
                rows = rows + (xs[plan[0, 1], own].astype(f32) + b_out[...])
            sect_src[1 + n, at] = rows.astype(bf16)
        act_parts[n][i].start()

    def each_soon(core_of, far_ones, job):
        for n in (0, 1):
            is_far = highs[n] * 2 + core_of == x_far
            pl.when(is_far if far_ones else jnp.logical_not(is_far))(lambda n=n: job(n, 0))

    def grad_pair():
        for h in (0, 1):
            pair_src[0, h] = total_rows(0, h, 1 - core).astype(bf16)
        pair_sum.start()

    def norm_stats():
        stat_send(0, 1, stat_total(0, 0))

    def normalize():
        total = unpack(stat_total(0, 1)) / D
        mean_f, mean_b = total[:, 0:1], total[:, 2:3]
        inv_f = lax.rsqrt(total[:, 1:2] - mean_f * mean_f + epsilon)
        inv_b = lax.rsqrt(total[:, 3:4] - mean_b * mean_b + epsilon)
        stats[0] = jnp.broadcast_to(mean_b, (rows, rows))
        stats[1] = jnp.broadcast_to(inv_b, (rows, rows))
        values = xs[plan[0, 1]].astype(f32)
        lhs[1, 0, mine] = ((values - mean_f) * inv_f * gain[...]).astype(bf16)
        normed_to_mate.start()
        normed_to_far.start()

    def normed_forward():
        normed_to_far.wait_recv_into(normed_rows.at[far_rows])
        normed_on.start()

    def normed_done():
        normed_to_mate.wait_recv()
        normed_on.wait_recv()
        for r in (row, mate_row, far_row, far_mate_row):
            swap_rows(1, r)
        for c in (normed_to_mate, normed_to_far, normed_on):
            c.wait_send()

    def grad_far():
        pair_sum.wait_recv()
        own_sum[...] = chip_rows(0, high)
        far_src[...] = chip_rows(0, 1 - high).astype(bf16)
        far_sum.start()
        pair_sum.wait_send()

    def hat():
        return (xs[plan[0, 0]].astype(f32) - stats[0, :, 0:1]) * stats[1, :, 0:1]

    def grad_stats():
        far_sum.wait_recv()
        scaled = (own_sum[...] + far_in[...].astype(f32)) * gain[...]
        own_sum[...] = scaled
        stat_send(1, 0, pack([row_sum(scaled), row_sum(scaled * hat())]))
        far_sum.wait_send()

    def grad_stats_more():
        stat_send(1, 1, stat_total(1, 0))

    def grad_out():
        total = unpack(stat_total(1, 1)) / D
        in_grad = grad[0].astype(f32) + stats[1, :, 0:1] * (
            own_sum[...] - total[:, 0:1] - hat() * total[:, 1:2]
        )
        sect_src[0] = in_grad.astype(bf16)
        grad_on.start()

    last = n_pair + len(stages) - 2
    early = (2, 4, 7, 9) if n_pair >= 10 else (1, 2, 4, 5)
    jobs = (
        (0, 0, first_stats),
        (1, 0, front_sent),
        (3, 3, loads[-1].wait),
        (early[0], 0, norm_stats),
        (early[1], 0, normalize),
        (early[2], 0, normed_forward),
        (early[3], 0, normed_done),
        (last, 8, grad_pair),
        (last + 1, 3, grad_far),
        (last + 3, 3, grad_stats),
        (last + 4, 0, grad_stats_more),
        (last + 4, 7, grad_out),
        (units + 6, 8, lambda: each_soon(1 - core, False, act_pair)),
        (units + 7, 7, lambda: each_soon(core, False, act_out)),
    )

    @pl.loop(0, units + len(stages) - 1)
    def _(step):
        for k, stage in enumerate(stages):
            u = step - k

            @pl.when(jnp.logical_and(u >= 0, u < units))
            def _():
                for q in (0, 1):
                    stage(u, q)

            for at, after, job in jobs:
                if after == k:
                    pl.when(step == at)(job)

    each_soon(1 - core, True, act_pair)
    for n in (0, 1):
        act_pair(n, 1)
    each_soon(core, True, act_out)
    for n in (0, 1):
        act_out(n, 1)
    grad_on.wait_recv()
    grad_recv[0] = sect_in[0]
    for i in (0, 1):
        for n in (0, 1):
            act_parts[n][i].wait_recv()
        for j in ((0, 1, 2), (3,))[i]:
            at = pl.ds(j * BLK, BLK)
            own = pl.ds(pl.multiple_of(turns[j] * BLK, BLK), BLK)
            act_recv[0, own] = (sect_in[1, at].astype(f32) + sect_in[2, at].astype(f32)).astype(bf16)
    for c in sum(pair_parts + act_parts, []) + [grad_on]:
        c.wait_send()


def store_kernel(*refs):
    n = len(refs) // 2
    copies = [
        pltpu.make_async_copy(refs[i], refs[n + i], refs[-1].at[i]) for i in range(n)
    ]
    for c in copies:
        c.start()
    for c in copies:
        c.wait()


def body(stash_inputs, stash_hidden, grad_in, w_in, b_in, w_out, b_out, ln_gain, plan, ft=FT):
    _, feat, hid = w_in.shape
    slots = stash_inputs.shape[1]
    tiles = hid // ft
    rows, mine = SIDE * SIDE * BLK, SIDE * BLK
    bf16, f32 = jnp.bfloat16, jnp.float32
    vmem, anyw = pl.BlockSpec(memory_space=pltpu.VMEM), pl.BlockSpec(memory_space=pl.ANY)
    results = pl.pallas_call(
        step_kernel,
        out_shape=(
            pltpu.VMEM((1, mine, feat), bf16),
            pltpu.VMEM((1, mine, feat), bf16),
            pltpu.VMEM((1, BLK, hid), bf16),
        ),
        in_specs=[pl.BlockSpec(memory_space=pltpu.SMEM)] + [anyw] * 8,
        out_specs=(vmem, vmem, vmem),
        scratch_shapes=[
            *(pltpu.VMEM(v.shape, v.dtype) for v in (grad_in, ln_gain, b_in, b_out)),
            pltpu.VMEM((2, 2, rows, feat), bf16),
            pltpu.VMEM((slots, mine, feat), bf16),
            pltpu.VMEM((slots, BLK, hid), bf16),
            pltpu.VMEM((2, 2, 8, mine), f32),
            pltpu.VMEM((2, 2, 3, 8, mine), f32),
            pltpu.VMEM((2, mine, mine), f32),
            pltpu.VMEM((2, 2, mine, feat), bf16),
            pltpu.VMEM((2, 2, mine, feat), bf16),
            pltpu.VMEM((PIECES, mine // PIECES, feat), bf16),
            pltpu.VMEM((mine, feat), f32),
            pltpu.VMEM((mine, feat), bf16),
            pltpu.VMEM((mine, feat), bf16),
            pltpu.VMEM((3, mine, feat), bf16),
            pltpu.VMEM((3, mine, feat), bf16),
            pltpu.VMEM((tiles, feat, ft), bf16),
            pltpu.VMEM((tiles, ft, feat), bf16),
            pltpu.VMEM((2, LOCAL, rows, ft), bf16),
            pltpu.VMEM((2, SLOTS, 2, 2 * BLK, ft), bf16),
            pltpu.VMEM((2, SLOTS, 2, 4 * BLK, ft), bf16),
            pltpu.VMEM((2, LOCAL, 4 * BLK, ft), bf16),
            pltpu.VMEM((2, SLOTS, 2, BLK // 2, ft), bf16),
            pltpu.VMEM((2, SLOTS, 2, BLK, ft), bf16),
            pltpu.VMEM((2, SLOTS, SIDE, SIDE, BLK, ft), bf16),
            pltpu.VMEM((2, 2, rows, feat), f32),
            pltpu.SemaphoreType.DMA((4, 2, LOCAL)),
            pltpu.SemaphoreType.DMA((8, 2, SLOTS)),
            pltpu.SemaphoreType.DMA((tiles,)),
            pltpu.SemaphoreType.DMA((tiles,)),
            pltpu.SemaphoreType.DMA((6,)),
            pltpu.SemaphoreType.DMA((FRONT + 3 * PIECES + 8,)),
            pltpu.SemaphoreType.DMA((FRONT + 3 * PIECES + 8,)),
        ],
        compiler_params=pltpu.CompilerParams(
            collective_id=0, has_side_effects=True, vmem_limit_bytes=60 << 20
        ),
        name="section_step",
    )(plan, grad_in, ln_gain, b_in, b_out, stash_inputs, stash_hidden, w_in, w_out)
    return pl.pallas_call(
        store_kernel,
        out_shape=tuple(jax.ShapeDtypeStruct(r.shape, r.dtype) for r in results),
        in_specs=[vmem] * 3,
        out_specs=(anyw,) * 3,
        scratch_shapes=[pltpu.SemaphoreType.DMA((3,))],
        compiler_params=pltpu.CompilerParams(vmem_limit_bytes=4 << 20),
        name="store",
    )(*results)


def solution(mesh):
    in_specs = (
        P("section", None, "row", "col"),
        P("section", None, "col", "row"),
        P("section", "row", "col"),
        P("section", "col", "row"),
        P("section", "row"),
        P("section", "row", "col"),
        P("section", "col"),
        P("section", "col"),
        P("section", None),
    )
    out_specs = (P("section", "row", "col"), P("section", "row", "col"), P("section", "col", "row"))
    return jax.shard_map(body, mesh=mesh, in_specs=in_specs, out_specs=out_specs, check_vma=False)
```

```python
import jax
import jax.numpy as jnp
from jax import lax
from jax.experimental import pallas as pl
from jax.experimental.pallas import tpu as pltpu
from jax.sharding import PartitionSpec as P

D = 12288
FT = 512
SIDE = 4
SLOTS = 8
LOCAL = 4
BLK = 32
LATE_STAGE = 8
PIECES = 4
FRONT = 32

epsilon = 1e-05
root_coef = 0.7978845608028654
cubic_coef = 0.044715

RB1, LR1, RB2, LR2, A1, AR1, A2, AR2 = range(8)
SEND_RING = (0, 0, 1, 1, 2, 2, 3, 3)


def gelu_value(values):
    inner = root_coef * (values + cubic_coef * values * values * values)
    return 0.5 * values * (1.0 + jnp.tanh(inner))


def gelu_slope(values):
    inner = root_coef * (values + cubic_coef * values * values * values)
    tangent = jnp.tanh(inner)
    return 0.5 * (1.0 + tangent) + 0.5 * values * (1.0 - tangent * tangent) * root_coef * (
        1.0 + 3.0 * cubic_coef * values * values
    )


def dot_nn(a, b):
    return jnp.dot(a, b, preferred_element_type=jnp.float32)


def dot_nt(a, b):
    return lax.dot_general(a, b, (((1,), (1,)), ((), ())), preferred_element_type=jnp.float32)


class Copy:
    def __init__(self, *args):
        self.args = args

    def make(self):
        src, dst, send, recv, dev = self.args
        return pltpu.make_async_remote_copy(
            src_ref=src,
            dst_ref=dst,
            send_sem=send,
            recv_sem=recv,
            device_id=dev,
            device_id_type=pl.DeviceIdType.MESH,
        )

    def start(self):
        self.make().start()

    def wait_recv(self):
        self.make().wait_recv()

    def wait_recv_into(self, dst):
        src, _, send, recv, dev = self.args
        Copy(dst, dst, send, recv, dev).wait_recv()

    def wait_send(self):
        self.make().wait_send()


def step_kernel(
    plan,
    grad_h,
    gain_h,
    b_in_h,
    b_out_h,
    stash_x,
    stash_h,
    w_in,
    w_out,
    act_recv,
    grad_recv,
    saved,
    grad,
    gain,
    b_in,
    b_out,
    lhs,
    xs,
    stash,
    stat_src,
    stat_in,
    stats,
    pair_src,
    pair_in,
    relay_in,
    own_sum,
    far_src,
    far_in,
    sect_src,
    sect_in,
    win_s,
    wout_s,
    parts,
    rb1,
    lr1,
    quart,
    rb2,
    lr2,
    gath,
    acc,
    send_sem,
    recv_sem,
    win_sem,
    wout_sem,
    load_sem,
    side_send,
    side_recv,
):
    n_pair = win_s.shape[0] // 2
    ft = win_s.shape[2]
    units = 2 * n_pair
    f32, bf16 = jnp.float32, jnp.bfloat16
    col = lax.axis_index("col")
    pos = (col // SIDE, lax.rem(col, SIDE))

    def wrap(v):
        return jnp.bitwise_and(v + SIDE, SIDE - 1)

    along = (
        [{"col": wrap(pos[0] + by) * SIDE + pos[1]} for by in (1, 2, 3)],
        [{"col": pos[0] * SIDE + wrap(pos[1] + by)} for by in (1, 2, 3)],
    )
    hops = tuple((ring[0], ring[2]) for ring in along)
    places = tuple((p, wrap(p + 1), wrap(p + 2), wrap(p + 3)) for p in pos)

    def slot(u):
        return jnp.bitwise_and(u, SLOTS - 1)

    def local(u):
        return jnp.bitwise_and(u, LOCAL - 1)

    def win_copy(t):
        return pltpu.make_async_copy(
            w_in.at[0, :, pl.ds(pl.multiple_of(t * ft, ft), ft)], win_s.at[t], win_sem.at[t]
        )

    def wout_copy(t):
        return pltpu.make_async_copy(
            w_out.at[0, pl.ds(pl.multiple_of(t * ft, ft), ft), :], wout_s.at[t], wout_sem.at[t]
        )

    rows = SIDE * BLK
    feat = win_s.shape[1]
    row = lax.axis_index("row")
    high, core = row // 2, lax.rem(row, 2)
    section = lax.axis_index("section")
    mate = {"row": high * 2 + 1 - core}
    far = {"row": (1 - high) * 2 + core}
    next_same = {"section": 1 - section, "row": row}
    next_far = {"section": 1 - section, "row": (1 - high) * 2 + core}
    everyone = [*along[0], *along[1], mate, far, next_same, next_far]

    def side(i, src, dst, dev):
        return Copy(src, dst, side_send.at[i], side_recv.at[i], dev)

    barrier = pltpu.get_barrier_semaphore()
    for dev in everyone:
        pl.semaphore_signal(barrier, inc=1, device_id=dev, device_id_type=pl.DeviceIdType.MESH)

    loads = [
        pltpu.make_async_copy(src, dst, load_sem.at[i])
        for i, (src, dst) in enumerate(
            (
                (grad_h, grad),
                (stash_x.at[0], xs),
                (gain_h, gain),
                (b_in_h, b_in),
                (b_out_h, b_out),
                (stash_h.at[0], stash),
            )
        )
    ]
    for c in loads[:-1]:
        c.start()

    @pl.loop(0, 2 * n_pair)
    def _(t):
        wout_copy(t).start()

    loads[-1].start()

    @pl.loop(0, 2 * n_pair)
    def _(t):
        win_copy(t).start()

    pl.semaphore_wait(barrier, len(everyone))
    loads[0].wait()

    def row_block(high_of, core_of):
        return pl.ds(pl.multiple_of((high_of * 2 + core_of) * rows, rows), rows)

    piece = rows // PIECES
    mine, far_rows = row_block(high, core), row_block(1 - high, core)
    grads = lhs.at[0, 0]

    def piece_of(block_high, n):
        return pl.ds(pl.multiple_of((block_high * 2 + core) * rows + n * piece, piece), piece)

    by_way = (next_same, next_far)
    to_mate = side(0, grad.at[0], grads.at[mine], mate)
    out_hops = [
        side(FRONT + n, grad.at[0, pl.ds(n * piece, piece)], relay_in.at[n], by_way[n % 2])
        for n in range(PIECES)
    ]
    on_hops = [
        side(
            FRONT + PIECES + n,
            relay_in.at[n],
            grads.at[piece_of((high, 1 - high)[n % 2], n)],
            by_way[1 - n % 2],
        )
        for n in range(PIECES)
    ]
    far_to_mate = [
        side(
            FRONT + 2 * PIECES + n,
            grads.at[piece_of(1 - high, n)],
            grads.at[piece_of(1 - high, n)],
            mate,
        )
        for n in range(PIECES)
    ]
    for c in out_hops + [to_mate]:
        c.start()
    lhs[0, 0, mine] = grad[0]
    for n in range(PIECES):
        out_hops[n].wait_recv()
        on_hops[n].start()

    def pack(columns):
        lane = lax.broadcasted_iota(jnp.int32, (rows, rows), 1)
        grid = jnp.zeros((rows, rows), f32)
        for i, c in enumerate(columns):
            grid = jnp.where(lane == i, c, grid)
        return grid.T[:8]

    def unpack(packed):
        return jnp.concatenate([packed] * (rows // 8), axis=0).T

    def stat_copies(n, axis):
        first = 8 + (2 * n + axis) * 3
        return [
            side(first + j - 1, stat_src.at[n, axis], stat_in.at[n, axis, j - 1], along[axis][j - 1])
            for j in (1, 2, 3)
        ]

    def stat_send(n, axis, value):
        stat_src[n, axis] = value
        for c in stat_copies(n, axis):
            c.start()

    def stat_total(n, axis):
        copies = stat_copies(n, axis)
        for c in copies:
            c.wait_recv()
        total = stat_src[n, axis]
        for j in (0, 1, 2):
            total = total + stat_in[n, axis, j]
        for c in copies:
            c.wait_send()
        return total

    def row_sum(v):
        return jnp.sum(v, axis=1, keepdims=True)

    def first_stats():
        for c in loads[1:-1]:
            c.wait()
        fwd_input = xs[plan[0, 1]].astype(f32)
        bwd_input = xs[plan[0, 0]].astype(f32)
        sums = [
            row_sum(fwd_input),
            row_sum(fwd_input * fwd_input),
            row_sum(bwd_input),
            row_sum(bwd_input * bwd_input),
        ]
        stat_send(0, 0, pack(sums))

    def swap_rows(k, r):
        for z in range(SIDE):
            lhs[k, 1, pl.ds(pl.multiple_of((z * SIDE + r) * BLK, BLK), BLK)] = lhs[
                k, 0, pl.ds(pl.multiple_of((r * SIDE + z) * BLK, BLK), BLK)
            ]

    far_row = (1 - high) * 2 + core
    mate_row, far_mate_row = high * 2 + 1 - core, (1 - high) * 2 + 1 - core
    swap_rows(0, row)
    to_mate.wait_recv()
    swap_rows(0, mate_row)
    for n in range(PIECES):
        on_hops[n].wait_recv_into(grads.at[piece_of(1 - high, n)])
        far_to_mate[n].start()
    swap_rows(0, far_row)
    for n in range(PIECES):
        far_to_mate[n].wait_recv()
    swap_rows(0, far_mate_row)

    def front_sent():
        for c in out_hops + on_hops + far_to_mate + [to_mate]:
            c.wait_send()

    def ring(q, phase):
        axis = (q + phase) % 2
        return places[axis], hops[axis]

    def copy(kind, q, u, d, src, dst, hop):
        return Copy(
            src,
            dst,
            send_sem.at[SEND_RING[kind], q, local(u)],
            recv_sem.at[kind, q, slot(u)],
            hop[d],
        )

    def arrived(kind, q, u, ref):
        Copy(ref, ref, send_sem.at[0, q, 0], recv_sem.at[kind, q, slot(u)], hops[0][0]).wait_recv()

    def all_sent(ring_no, q, u, ref):
        Copy(ref, ref, send_sem.at[ring_no, q, local(u)], recv_sem.at[0, q, 0], hops[0][0]).wait_send()

    def span(i, size, lo, n):
        return pl.ds(pl.multiple_of(i * size + lo, n), n)

    def scatter_first(buf, back, side_buf, size, kinds, place, hop, q, u):
        half = size // 2
        me, nxt, far_one, prv = place
        src, s = buf.at[q, local(u)], slot(u)
        copy(kinds[0], q, u, 0, src.at[span(far_one, size, 0, half)], back.at[q, s, 0], hop).start()
        copy(kinds[0], q, u, 1, src.at[span(far_one, size, half, half)], back.at[q, s, 1], hop).start()
        copy(kinds[1], q, u, 0, src.at[span(nxt, size, half, half)],
             side_buf.at[q, s, 0, pl.ds(half, half)], hop).start()
        copy(kinds[1], q, u, 1, src.at[span(prv, size, 0, half)],
             side_buf.at[q, s, 1, pl.ds(0, half)], hop).start()

    def scatter_relay(buf, back, side_buf, size, kinds, place, hop, q, u):
        half = size // 2
        me, nxt, far_one, prv = place
        l, s = local(u), slot(u)
        arrived(kinds[0], q, u, back.at[q, s])
        for d, (chunk, lo) in enumerate(((nxt, 0), (prv, half))):
            rows = span(chunk, size, lo, half)
            buf[q, l, rows] = (
                buf[q, l, rows].astype(f32) + back[q, s, d].astype(f32)
            ).astype(bf16)
            copy(kinds[1], q, u, d, buf.at[q, l, rows],
                 side_buf.at[q, s, d, pl.ds(lo, half)], hop).start()

    big, small = SIDE * BLK, BLK

    def s0(u, q):
        l = local(u)

        @pl.when(u < n_pair)
        def _():
            t = 2 * u + q
            wout_copy(t).wait()
            parts[q, l] = dot_nt(lhs[0, q], wout_s[t]).astype(bf16)

        @pl.when(u >= n_pair)
        def _():
            t = 2 * (u - n_pair) + q
            if n_pair < LATE_STAGE - 1:
                win_copy(t).wait()
            parts[q, l] = dot_nn(lhs[1, q], win_s[t]).astype(bf16)

        scatter_first(parts, rb1, lr1, big, (RB1, LR1), *ring(q, 0), q, u)

    def s1(u, q):
        scatter_relay(parts, rb1, lr1, big, (RB1, LR1), *ring(q, 0), q, u)

    def s2(u, q):
        place, _ = ring(q, 0)
        l, s = local(u), slot(u)
        arrived(LR1, q, u, lr1.at[q, s])
        quart[q, l] = (
            parts[q, l, span(place[0], big, 0, big)].astype(f32)
            + lr1[q, s, 0].astype(f32)
            + lr1[q, s, 1].astype(f32)
        ).astype(bf16)
        scatter_first(quart, rb2, lr2, small, (RB2, LR2), *ring(q, 1), q, u)
        all_sent(0, q, u, parts.at[q, l, pl.ds(0, 3 * big)])

    def s3(u, q):
        scatter_relay(quart, rb2, lr2, small, (RB2, LR2), *ring(q, 1), q, u)

    def s4(u, q):
        me1 = ring(q, 0)[0][0]
        place, hop = ring(q, 1)
        me2 = place[0]
        l, s = local(u), slot(u)
        arrived(LR2, q, u, lr2.at[q, s])
        h = (
            quart[q, l, span(me2, small, 0, small)].astype(f32)
            + lr2[q, s, 0].astype(f32)
            + lr2[q, s, 1].astype(f32)
        )

        @pl.when(u < n_pair)
        def _():
            t = 2 * u + q
            cols = pl.ds(pl.multiple_of(t * ft, ft), ft)
            slope = gelu_slope(stash[plan[0, 0], :, cols].astype(f32))
            gath[q, s, me1, me2] = (h * slope).astype(bf16)

        @pl.when(u >= n_pair)
        def _():
            t = 2 * (u - n_pair) + q
            cols = pl.ds(pl.multiple_of(t * ft, ft), ft)
            hidden = h + b_in[:, cols]
            saved[0, :, cols] = hidden.astype(bf16)
            gath[q, s, me1, me2] = gelu_value(hidden).astype(bf16)

        g = gath.at[q, s, me1, me2]
        for d in (0, 1):
            copy(A1, q, u, d, g, g, hop).start()
        all_sent(1, q, u, quart.at[q, l, pl.ds(0, 3 * small)])

    def s5(u, q):
        me1 = ring(q, 0)[0][0]
        place, hop = ring(q, 1)
        g = gath.at[q, slot(u), me1]
        arrived(A1, q, u, g.at[pl.ds(0, 2)])
        for d, (b, lo) in enumerate(((place[3], 0), (place[1], BLK // 2))):
            r = g.at[b, pl.ds(lo, BLK // 2)]
            copy(AR1, q, u, d, r, r, hop).start()

    def product(u, q, blocks):
        s = slot(u)

        def add(kind, first, values):
            @pl.when(first)
            def _():
                for b, value in zip(blocks, values):
                    acc[kind, q, span(b, big, 0, big)] = value

            @pl.when(jnp.logical_not(first))
            def _():
                for b, value in zip(blocks, values):
                    acc[kind, q, span(b, big, 0, big)] += value

        pieces = [gath[q, s, b].reshape(big, ft) for b in blocks]

        @pl.when(u < n_pair)
        def _():
            t = 2 * u + q
            add(0, u == 0, [dot_nt(piece, win_s[t]) for piece in pieces])

        @pl.when(u >= n_pair)
        def _():
            t = 2 * (u - n_pair) + q
            add(1, u == n_pair, [dot_nn(piece, wout_s[t]) for piece in pieces])

    def s6(u, q):
        place, hop = ring(q, 0)
        me1 = place[0]
        g = gath.at[q, slot(u)]
        arrived(AR1, q, u, g.at[me1, 0])
        for d in (0, 1):
            copy(A2, q, u, d, g.at[me1], g.at[me1], hop).start()
        if n_pair >= LATE_STAGE - 1:

            @pl.when(u < n_pair)
            def _():
                win_copy(2 * u + q).wait()

        product(u, q, [me1])
        all_sent(2, q, u, g.at[me1, pl.ds(0, 3)])

    def s7(u, q):
        place, hop = ring(q, 0)
        g = gath.at[q, slot(u)]
        arrived(A2, q, u, g.at[pl.ds(0, 2)])
        for d, (b, lo) in enumerate(((place[3], 0), (place[1], SIDE // 2))):
            r = g.at[b, pl.ds(lo, SIDE // 2)]
            copy(AR2, q, u, d, r, r, hop).start()
        product(u, q, [place[1], place[3]])

    def s8(u, q):
        place, _ = ring(q, 0)
        g = gath.at[q, slot(u)]
        arrived(AR2, q, u, g.at[0])
        product(u, q, [place[2]])
        all_sent(3, q, u, g.at[pl.ds(0, 3)])

    stages = (s0, s1, s2, s3, s4, s5, s6, s7, s8)
    normed_rows = lhs.at[1, 0]
    base = 20
    normed_to_mate = side(base, normed_rows.at[mine], normed_rows.at[mine], mate)
    normed_to_far = side(base + 1, normed_rows.at[mine], normed_rows.at[mine], far)
    normed_on = side(base + 2, normed_rows.at[far_rows], normed_rows.at[far_rows], mate)
    pair_sum = side(base + 3, pair_src.at[0], pair_in.at[0], mate)
    far_sum = side(base + 5, far_src, far_in, far)
    grad_on = side(base + 6, sect_src.at[0], sect_in.at[0], next_same)
    tail = FRONT + 3 * PIECES
    x_far = places[0][2]
    turns = tuple(places[1][i] for i in (0, 1, 3, 2))
    soon, late = pl.ds(0, 3 * BLK), pl.ds(3 * BLK, BLK)
    highs = (high, 1 - high)
    pair_parts = [
        [
            side(tail + 2 * n + i, pair_src.at[1, n, r], pair_in.at[1, n, r], mate)
            for i, r in enumerate((soon, late))
        ]
        for n in (0, 1)
    ]
    act_parts = [
        [
            side(tail + 4 + 2 * n + i, sect_src.at[1 + n, r], sect_in.at[1 + n, r], by_way[n])
            for i, r in enumerate((soon, late))
        ]
        for n in (0, 1)
    ]

    def token_rows(k, r, z):
        own = pl.ds(pl.multiple_of((r * SIDE + z) * BLK, BLK), BLK)
        swap = pl.ds(pl.multiple_of((z * SIDE + r) * BLK, BLK), BLK)
        return acc[k, 0, own] + acc[k, 1, swap]

    def total_rows(k, high_of, core_of):
        r = high_of * 2 + core_of
        return jnp.concatenate([token_rows(k, r, z) for z in range(SIDE)], axis=0)

    def chip_rows(k, high_of):
        return total_rows(k, high_of, core) + pair_in[k, high_of].astype(f32)

    def act_pair(n, i):
        for j in ((0, 1, 2), (3,))[i]:
            rows = token_rows(1, highs[n] * 2 + 1 - core, turns[j])
            pair_src[1, n, pl.ds(j * BLK, BLK)] = rows.astype(bf16)
        pair_parts[n][i].start()

    def act_out(n, i):
        pair_parts[n][i].wait_recv()
        for j in ((0, 1, 2), (3,))[i]:
            at = pl.ds(j * BLK, BLK)
            rows = token_rows(1, highs[n] * 2 + core, turns[j]) + pair_in[1, n, at].astype(f32)
            if n == 0:
                own = pl.ds(pl.multiple_of(turns[j] * BLK, BLK), BLK)
                rows = rows + (xs[plan[0, 1], own].astype(f32) + b_out[...])
            sect_src[1 + n, at] = rows.astype(bf16)
        act_parts[n][i].start()

    def each_soon(core_of, far_ones, job):
        for n in (0, 1):
            is_far = highs[n] * 2 + core_of == x_far
            pl.when(is_far if far_ones else jnp.logical_not(is_far))(lambda n=n: job(n, 0))

    def grad_pair():
        for h in (0, 1):
            pair_src[0, h] = total_rows(0, h, 1 - core).astype(bf16)
        pair_sum.start()

    def norm_stats():
        stat_send(0, 1, stat_total(0, 0))

    def normalize():
        total = unpack(stat_total(0, 1)) / D
        mean_f, mean_b = total[:, 0:1], total[:, 2:3]
        inv_f = lax.rsqrt(total[:, 1:2] - mean_f * mean_f + epsilon)
        inv_b = lax.rsqrt(total[:, 3:4] - mean_b * mean_b + epsilon)
        stats[0] = jnp.broadcast_to(mean_b, (rows, rows))
        stats[1] = jnp.broadcast_to(inv_b, (rows, rows))
        values = xs[plan[0, 1]].astype(f32)
        lhs[1, 0, mine] = ((values - mean_f) * inv_f * gain[...]).astype(bf16)
        normed_to_mate.start()
        normed_to_far.start()

    def normed_forward():
        normed_to_far.wait_recv_into(normed_rows.at[far_rows])
        normed_on.start()

    def normed_done():
        normed_to_mate.wait_recv()
        normed_on.wait_recv()
        for r in (row, mate_row, far_row, far_mate_row):
            swap_rows(1, r)
        for c in (normed_to_mate, normed_to_far, normed_on):
            c.wait_send()

    def grad_far():
        pair_sum.wait_recv()
        own_sum[...] = chip_rows(0, high)
        far_src[...] = chip_rows(0, 1 - high).astype(bf16)
        far_sum.start()
        pair_sum.wait_send()

    def hat():
        return (xs[plan[0, 0]].astype(f32) - stats[0, :, 0:1]) * stats[1, :, 0:1]

    def grad_stats():
        far_sum.wait_recv()
        scaled = (own_sum[...] + far_in[...].astype(f32)) * gain[...]
        own_sum[...] = scaled
        stat_send(1, 0, pack([row_sum(scaled), row_sum(scaled * hat())]))
        far_sum.wait_send()

    def grad_stats_more():
        stat_send(1, 1, stat_total(1, 0))

    def grad_out():
        total = unpack(stat_total(1, 1)) / D
        in_grad = grad[0].astype(f32) + stats[1, :, 0:1] * (
            own_sum[...] - total[:, 0:1] - hat() * total[:, 1:2]
        )
        sect_src[0] = in_grad.astype(bf16)
        grad_on.start()

    last = n_pair + len(stages) - 2
    early = (2, 4, 7, 9) if n_pair >= 10 else (2, 3, 4, 5)
    jobs = (
        (1, 1, first_stats),
        (1, 0, front_sent),
        (3, 3, loads[-1].wait),
        (early[0], 0, norm_stats),
        (early[1], 0, normalize),
        (early[2], 4, normed_forward),
        (early[3], 0, normed_done),
        (last, 8, grad_pair),
        (last + 1, 3, grad_far),
        (last + 3, 3, grad_stats),
        (last + 4, 0, grad_stats_more),
        (last + 4, 7, grad_out),
        (units + 6, 8, lambda: each_soon(1 - core, False, act_pair)),
        (units + 7, 7, lambda: each_soon(core, False, act_out)),
    )

    @pl.loop(0, units + len(stages) - 1)
    def _(step):
        for k, stage in enumerate(stages):
            u = step - k

            @pl.when(jnp.logical_and(u >= 0, u < units))
            def _():
                for q in (0, 1):
                    stage(u, q)

            for at, after, job in jobs:
                if after == k:
                    pl.when(step == at)(job)

    each_soon(1 - core, True, act_pair)
    for n in (0, 1):
        act_pair(n, 1)
    each_soon(core, True, act_out)
    for n in (0, 1):
        act_out(n, 1)
    grad_on.wait_recv()
    grad_recv[0] = sect_in[0]
    for i in (0, 1):
        for n in (0, 1):
            act_parts[n][i].wait_recv()
        for j in ((0, 1, 2), (3,))[i]:
            at = pl.ds(j * BLK, BLK)
            own = pl.ds(pl.multiple_of(turns[j] * BLK, BLK), BLK)
            act_recv[0, own] = (sect_in[1, at].astype(f32) + sect_in[2, at].astype(f32)).astype(bf16)
    for c in sum(pair_parts + act_parts, []) + [grad_on]:
        c.wait_send()


def store_kernel(*refs):
    n = len(refs) // 2
    copies = [
        pltpu.make_async_copy(refs[i], refs[n + i], refs[-1].at[i]) for i in range(n)
    ]
    for c in copies:
        c.start()
    for c in copies:
        c.wait()


def body(stash_inputs, stash_hidden, grad_in, w_in, b_in, w_out, b_out, ln_gain, plan, ft=FT):
    _, feat, hid = w_in.shape
    slots = stash_inputs.shape[1]
    tiles = hid // ft
    rows, mine = SIDE * SIDE * BLK, SIDE * BLK
    bf16, f32 = jnp.bfloat16, jnp.float32
    vmem, anyw = pl.BlockSpec(memory_space=pltpu.VMEM), pl.BlockSpec(memory_space=pl.ANY)
    results = pl.pallas_call(
        step_kernel,
        out_shape=(
            pltpu.VMEM((1, mine, feat), bf16),
            pltpu.VMEM((1, mine, feat), bf16),
            pltpu.VMEM((1, BLK, hid), bf16),
        ),
        in_specs=[pl.BlockSpec(memory_space=pltpu.SMEM)] + [anyw] * 8,
        out_specs=(vmem, vmem, vmem),
        scratch_shapes=[
            *(pltpu.VMEM(v.shape, v.dtype) for v in (grad_in, ln_gain, b_in, b_out)),
            pltpu.VMEM((2, 2, rows, feat), bf16),
            pltpu.VMEM((slots, mine, feat), bf16),
            pltpu.VMEM((slots, BLK, hid), bf16),
            pltpu.VMEM((2, 2, 8, mine), f32),
            pltpu.VMEM((2, 2, 3, 8, mine), f32),
            pltpu.VMEM((2, mine, mine), f32),
            pltpu.VMEM((2, 2, mine, feat), bf16),
            pltpu.VMEM((2, 2, mine, feat), bf16),
            pltpu.VMEM((PIECES, mine // PIECES, feat), bf16),
            pltpu.VMEM((mine, feat), f32),
            pltpu.VMEM((mine, feat), bf16),
            pltpu.VMEM((mine, feat), bf16),
            pltpu.VMEM((3, mine, feat), bf16),
            pltpu.VMEM((3, mine, feat), bf16),
            pltpu.VMEM((tiles, feat, ft), bf16),
            pltpu.VMEM((tiles, ft, feat), bf16),
            pltpu.VMEM((2, LOCAL, rows, ft), bf16),
            pltpu.VMEM((2, SLOTS, 2, 2 * BLK, ft), bf16),
            pltpu.VMEM((2, SLOTS, 2, 4 * BLK, ft), bf16),
            pltpu.VMEM((2, LOCAL, 4 * BLK, ft), bf16),
            pltpu.VMEM((2, SLOTS, 2, BLK // 2, ft), bf16),
            pltpu.VMEM((2, SLOTS, 2, BLK, ft), bf16),
            pltpu.VMEM((2, SLOTS, SIDE, SIDE, BLK, ft), bf16),
            pltpu.VMEM((2, 2, rows, feat), f32),
            pltpu.SemaphoreType.DMA((4, 2, LOCAL)),
            pltpu.SemaphoreType.DMA((8, 2, SLOTS)),
            pltpu.SemaphoreType.DMA((tiles,)),
            pltpu.SemaphoreType.DMA((tiles,)),
            pltpu.SemaphoreType.DMA((6,)),
            pltpu.SemaphoreType.DMA((FRONT + 3 * PIECES + 8,)),
            pltpu.SemaphoreType.DMA((FRONT + 3 * PIECES + 8,)),
        ],
        compiler_params=pltpu.CompilerParams(
            collective_id=0, has_side_effects=True, vmem_limit_bytes=60 << 20
        ),
        name="section_step",
    )(plan, grad_in, ln_gain, b_in, b_out, stash_inputs, stash_hidden, w_in, w_out)
    return pl.pallas_call(
        store_kernel,
        out_shape=tuple(jax.ShapeDtypeStruct(r.shape, r.dtype) for r in results),
        in_specs=[vmem] * 3,
        out_specs=(anyw,) * 3,
        scratch_shapes=[pltpu.SemaphoreType.DMA((3,))],
        compiler_params=pltpu.CompilerParams(vmem_limit_bytes=4 << 20),
        name="store",
    )(*results)


def solution(mesh):
    in_specs = (
        P("section", None, "row", "col"),
        P("section", None, "col", "row"),
        P("section", "row", "col"),
        P("section", "col", "row"),
        P("section", "row"),
        P("section", "row", "col"),
        P("section", "col"),
        P("section", "col"),
        P("section", None),
    )
    out_specs = (P("section", "row", "col"), P("section", "row", "col"), P("section", "col", "row"))
    return jax.shard_map(body, mesh=mesh, in_specs=in_specs, out_specs=out_specs, check_vma=False)
```
